512 devices in a mesh: owner: 128 (over x, z, core), replica: 4 (over y).
Axes of the slice: x: 4, y: 4, z: 16, core: 2. Of those that a mesh axis runs over, the one named last changes fastest.
Arguments:
- features: bfloat16 [32768, 4096], P('owner', 'replica'), may hold values from -6 to 6
- cotangent: bfloat16 [32768, 64], P('owner'), may hold values from -0.59765625 to 0.59765625
- adapter_ids: int32 [32768, 1], P('owner'), may hold values from 0 to 255; in each aligned block of 256 rows (0 to 255, 256 to 511, ...) at most 2 rows name the same one
- slot_of: int32 [256], replicated, may hold values from 0 to 255, each once
- active_ids: int32 [192], replicated, may hold values from 0 to 255, as said below
- step_counts: int32 [256], P('owner'), may hold values from 0 to 15
- weight: bfloat16 [256, 64, 4096], P('owner', None, 'replica'), may hold values from -0.09375 to 0.09375
- m_code: bfloat16 [256, 64, 4096], P('owner', None, 'replica'), may hold values from -1 to 1
- m_scale: float32 [256, 32, 4], P('owner', None, 'replica'), may hold values from 0.1 to 1
- v_code: bfloat16 [256, 64, 4096], P('owner', None, 'replica'), may hold values from 0.099609375 to 1
- v_scale: float32 [256, 32, 4], P('owner', None, 'replica'), may hold values from 0.1 to 2
Outputs:
- direction: float32 [256, 64, 4096], P('owner', None, 'replica')
- m_code_new: bfloat16 [256, 64, 4096], P('owner', None, 'replica')
- m_scale_new: float32 [256, 32, 4], P('owner', None, 'replica')
- v_code_new: bfloat16 [256, 64, 4096], P('owner', None, 'replica')
- v_scale_new: float32 [256, 32, 4], P('owner', None, 'replica')
- served: bfloat16 [256, 64, 4096], P('owner')
The draws below stay inside these ranges and needn't reach their ends.
Inputs may be any that keep to these rules, and one draw needn't show every extreme that they name: `adapter_ids`: among the 256 tokens of one index of owner no adapter is named more than 2 times. `slot_of`: A permutation. `active_ids`: distinct adapters.
All inputs are finite; a program needn't handle non-finite values.
Results may differ from the reference program's by a relative error of at most 0.001.
Values may be sent and summed in bfloat16 or wider, within the bound.
No kernel may reach another device: no remote copies, remote signals or barrier semaphores. Data moves between devices by JAX's collectives and lax.ppermute only.
A program may use at most 64 MiB of HBM per device.

```python
import math
import jax
import jax.numpy as jnp
import numpy as np
from jax import lax

D = 4096
R = 64
BLOCK_COLS = 1024
TOK_DEV = 256
ADAPTERS = 256
TOKENS = 32768
CAP = 2
ACTIVE = 192
N_OWNER = 128


def draw_active_ids(key, part):
    shuffled = jax.random.permutation(jax.random.fold_in(key, 17), ADAPTERS)
    return shuffled[:ACTIVE].astype(jnp.int32)


def set_ends(result, stream_key, least, top_value):
    longest = result.shape.index(max(result.shape))
    spots = []
    for shift in (0, 1):
        where = [jax.random.randint(jax.random.fold_in(stream_key, axis), (), 0, length) for axis, length in enumerate(result.shape)]
        where[longest] = (where[longest] + shift) % result.shape[longest]
        spots.append(tuple(where))
    return result.at[spots[0]].set(least).at[spots[1]].set(top_value)


def shard_levels(key, shape, cuts, least, top_value):
    def one(position, blocks):
        draws = jax.random.uniform(jax.random.fold_in(jax.random.fold_in(key, 6), position), (blocks,), jnp.float32, least / len(cuts), top_value / len(cuts))
        return jnp.repeat(jnp.exp(draws), shape[position] // blocks).reshape((-1,) + (1,) * (len(shape) - position - 1))

    loudness = one(*cuts[0])
    for cut in cuts[1:]:
        loudness = loudness * one(*cut)
    return loudness


def routed_block(key, own, number, rows, count, top, bound, slope):
    ranking = jax.random.permutation(key, count)
    packed, ordinary = shares(count, rows * top, bound, slope, True), shares(count, rows * top, bound, slope, False)
    places = jnp.arange(count)

    def named(tallies, offset_by):
        used = int((tallies > 0).sum())
        fixed = max(1, used // 4)
        passed = fixed + (places - fixed + offset_by * (used - fixed)) % max(1, count - fixed)
        return jnp.zeros((count,), jnp.int32).at[ranking[jnp.where(places < fixed, places, passed)]].set(jnp.asarray(tallies, jnp.int32))

    tallies = jnp.where(number % 4 == 0, named(packed, number // 4), named(ordinary, number - number // 4 - 1))
    mixed = jax.random.permutation(jax.random.fold_in(own, 3), count)
    donor, taker = mixed[0:count // 2 * 2:2], mixed[1:count // 2 * 2:2]
    margin = jnp.minimum(tallies[donor] - 1, bound - tallies[taker]) // 2
    margin = jnp.where((donor == ranking[0]) | (taker == ranking[0]) | (tallies[taker] == 0), 0, jnp.maximum(margin, 0))
    passed = jax.random.randint(jax.random.fold_in(own, 4), (count // 2,), 0, 1 << 20) % (margin + 1)
    tallies = tallies.at[donor].add(-passed).at[taker].add(passed)
    items = jnp.searchsorted(jnp.cumsum(tallies), jnp.arange(rows * top), side="right").astype(jnp.int32)
    grid = items.reshape(top, rows).T
    grid = grid[jax.random.permutation(jax.random.fold_in(own, 1), rows)]
    offset_by = jax.random.randint(jax.random.fold_in(own, 2), (rows, 1), 0, top)
    return jnp.take_along_axis(grid, (jnp.arange(top)[None, :] + offset_by) % top, axis=1)


def shares(number_of, total, bound, lean, full):
    weights = [(1 << 20) // math.isqrt(grade ** lean) + 1 for grade in range(1, number_of + 1)]
    largest = bound if full else min(bound, max(-(-total // number_of), total * weights[0] // sum(weights)))
    least = 1 if total - largest >= number_of - 1 else 0
    holding, rest = [largest] + [least] * (number_of - 1), total - largest - least * (number_of - 1)
    while rest > 0:
        movable = [i for i in range(1, number_of) if holding[i] < largest] or [i for i in range(1, number_of) if holding[i] < bound]
        whole, left = sum([weights[i] for i in movable]), rest
        for i in movable:
            addition = min(bound - holding[i], max(1, left * weights[i] // whole), rest)
            holding[i] = holding[i] + addition
            rest = rest - addition
    return np.array(holding)


def noise(stream_key, shape, deviation, reach, cuts=(), kind=jnp.bfloat16):
    drawn = deviation * jax.random.normal(stream_key, shape, jnp.float32)
    if cuts:
        drawn = drawn * shard_levels(stream_key, shape, cuts, -0.22, 0.18)
    return jnp.clip(drawn, -reach, reach).astype(kind)


def setup_inputs(seed: int = 0) -> dict:
    key_of = jax.random.split(jax.random.key(seed), 12)
    features = noise(key_of[0], (TOKENS, D), 1.0, 6.0, ((0, 128), (1, 4)))
    cotangent = noise(key_of[1], (TOKENS, R), 0.1, 0.59765625, ((0, 128),))
    adapter_ids_keys = jax.random.split(jax.random.fold_in(key_of[2], 1), TOKENS // TOK_DEV)
    adapter_ids_turns = jax.random.permutation(jax.random.fold_in(key_of[2], 3), TOKENS // TOK_DEV)
    adapter_ids = jax.vmap(lambda own, number: routed_block(jax.random.fold_in(key_of[2], 2), own, number, TOK_DEV, ADAPTERS, 1, CAP, 2))(adapter_ids_keys, adapter_ids_turns).reshape((TOKENS, 1))
    slot_of = jax.random.permutation(key_of[3], ADAPTERS).astype(jnp.int32)
    active_ids = draw_active_ids(jax.random.fold_in(key_of[11], 71), 0)
    step_counts = set_ends(jax.random.randint(key_of[5], (ADAPTERS,), 0, 16), jax.random.fold_in(key_of[5], 1), 0, 15).astype(jnp.int32)
    weight = noise(key_of[6], (ADAPTERS, R, D), D ** -0.5, 0.09375, ((0, 128), (2, 4)))
    m_code = jnp.clip(jax.random.uniform(key_of[7], (ADAPTERS, R, D), jnp.float32, -1.0, 1.0) * shard_levels(key_of[7], (ADAPTERS, R, D), ((0, 128), (2, 4)), -0.4, 0.0), -1.0, 1.0).astype(jnp.bfloat16)
    m_scale = jnp.clip(jnp.exp(math.log(1.0) - 2.3025851 * jax.random.uniform(key_of[8], (ADAPTERS, R // 2, D // BLOCK_COLS), jnp.float32) ** shard_levels(key_of[8], (ADAPTERS, R // 2, D // BLOCK_COLS), ((0, 128), (2, 4)), -0.2, 0.2)), 0.1, 1.0)
    v_code = jnp.clip(0.099609375 + 0.9003906 * jax.random.uniform(key_of[9], (ADAPTERS, R, D), jnp.float32) ** shard_levels(key_of[9], (ADAPTERS, R, D), ((0, 128), (2, 4)), -0.2, 0.2), 0.099609375, 1.0).astype(jnp.bfloat16)
    v_scale = jnp.clip(jnp.exp(math.log(2.0) - 2.9957323 * jax.random.uniform(key_of[10], (ADAPTERS, R // 2, D // BLOCK_COLS), jnp.float32) ** shard_levels(key_of[10], (ADAPTERS, R // 2, D // BLOCK_COLS), ((0, 128), (2, 4)), -0.2, 0.2)), 0.1, 2.0)
    return {"features": features, "cotangent": cotangent, "adapter_ids": adapter_ids, "slot_of": slot_of, "active_ids": active_ids, "step_counts": step_counts, "weight": weight, "m_code": m_code, "m_scale": m_scale, "v_code": v_code, "v_scale": v_scale}


beta_one = 0.9
beta_two = 0.999
adam_eps = 1e-08
scale_eps = 1e-06
learn_rate = 0.001
decay_rate = 0.01

def fill_index(slot_ids, capacity, slot_total):
    count_rows = slot_ids.shape[0]
    sorted_order = jnp.argsort(slot_ids, stable=True).astype(jnp.int32)
    ordered = slot_ids[sorted_order]
    group_first = jnp.searchsorted(ordered, ordered, side='left').astype(jnp.int32)
    group_rank = jnp.arange(count_rows, dtype=jnp.int32) - group_first
    in_group = jnp.zeros((count_rows,), jnp.int32).at[sorted_order].set(group_rank)
    target = slot_ids * capacity + in_group
    filler = jnp.full((slot_total * capacity,), count_rows, jnp.int32)
    return filler.at[target].set(jnp.arange(count_rows, dtype=jnp.int32))

def expand(scales):
    widened = jnp.repeat(scales, 2, axis=1)
    return jnp.repeat(widened, BLOCK_COLS, axis=2)

def block_max(values):
    shape = values.shape
    blocks = values.reshape(shape[0], shape[1] // 2, 2, shape[2] // BLOCK_COLS, BLOCK_COLS)
    return lax.optimization_barrier(jnp.max(jnp.abs(blocks), axis=(2, 4)))

def adam_update(gradient, weight, m_code, m_scale, v_code, v_scale, counts, active_flag):
    m_old = m_code.astype(jnp.float32) * expand(m_scale)
    v_old = v_code.astype(jnp.float32) * expand(v_scale)
    moment = beta_one * m_old + (1.0 - beta_one) * gradient
    second = beta_two * v_old + (1.0 - beta_two) * gradient * gradient
    count_f = (counts + 1).astype(jnp.float32)[:, None, None]
    m_hat = moment / (1.0 - jnp.power(beta_one, count_f))
    v_hat = second / (1.0 - jnp.power(beta_two, count_f))
    direction = m_hat / (jnp.sqrt(v_hat) + adam_eps)
    m_scale_new = block_max(moment) + scale_eps
    v_scale_new = block_max(second) + scale_eps
    m_code_new = (moment / expand(m_scale_new)).astype(jnp.bfloat16)
    v_code_new = (second / expand(v_scale_new)).astype(jnp.bfloat16)
    weight_f = weight.astype(jnp.float32)
    served = (weight_f - learn_rate * (direction + decay_rate * weight_f)).astype(jnp.bfloat16)
    keep = active_flag[:, None, None]
    direction = jnp.where(keep, direction, jnp.zeros_like(direction))
    m_code_new = jnp.where(keep, m_code_new, m_code)
    v_code_new = jnp.where(keep, v_code_new, v_code)
    m_scale_new = jnp.where(keep, m_scale_new, m_scale)
    v_scale_new = jnp.where(keep, v_scale_new, v_scale)
    served = jnp.where(keep, served, weight)
    return (direction, m_code_new, m_scale_new, v_code_new, v_scale_new, served)

def reference(features, cotangent, adapter_ids, slot_of, active_ids, step_counts, weight, m_code, m_scale, v_code, v_scale):
    feat_blocks = features.reshape(N_OWNER, TOK_DEV, D)
    cot_blocks = cotangent.reshape(N_OWNER, TOK_DEV, R)
    id_blocks = adapter_ids.reshape(N_OWNER, TOK_DEV)

    def accumulate(total, pieces):
        feat_block, cot_block, id_block = pieces
        slot_ids = slot_of[id_block].astype(jnp.int32)
        filler = fill_index(slot_ids, CAP, ADAPTERS)
        feat_pad = jnp.concatenate([feat_block, jnp.zeros((1, D), feat_block.dtype)], 0)
        cot_pad = jnp.concatenate([cot_block, jnp.zeros((1, R), cot_block.dtype)], 0)
        feat_rows = feat_pad[filler].astype(jnp.float32).reshape(ADAPTERS, CAP, D)
        cot_rows = cot_pad[filler].astype(jnp.float32).reshape(ADAPTERS, CAP, R)
        return (total + jnp.einsum('acr,acd->ard', cot_rows, feat_rows), None)
    start = jnp.zeros((ADAPTERS, R, D), jnp.float32)
    gradient, _ = lax.scan(accumulate, start, (feat_blocks, cot_blocks, id_blocks))
    active_slots = slot_of[active_ids]
    rows = jnp.arange(ADAPTERS, dtype=jnp.int32)
    active_flag = jnp.any(active_slots[:, None] == rows[None, :], axis=0)
    return adam_update(gradient, weight, m_code, m_scale, v_code, v_scale, step_counts, active_flag)
```

```python
import functools

import jax
import jax.numpy as jnp
from jax import lax
from jax.experimental import pallas as pl
from jax.experimental.pallas import tpu as pltpu
from jax.sharding import Mesh
from jax.sharding import PartitionSpec as P

beta_one = 0.9
beta_two = 0.999
adam_eps = 1e-08
scale_eps = 1e-06
learn_rate = 0.001
decay_rate = 0.01

LANES = 128
FIRST = 6
VMEM = pl.BlockSpec(memory_space=pltpu.VMEM)
SMEM = pl.BlockSpec(memory_space=pltpu.SMEM)


def message_rows(slots, blocks):
    rows = slots * blocks + slots // 2 + 1
    return -(-rows // 4) * 4


def iota(shape, dim):
    return lax.broadcasted_iota(jnp.int32, shape, dim)


def pack_kernel(slots, offset, core_ref, ids_ref, slot_ref, act_ref, feat_ref, cot_ref, out_ref, scr):
    tokens, columns = feat_ref.shape
    rank = cot_ref.shape[1]
    state_rows = slot_ref.shape[1]
    chips, tiles = out_ref.shape[0], out_ref.shape[1]
    rows, blocks = tiles * 4, columns // LANES
    f32, bf16 = jnp.float32, jnp.bfloat16
    dot = functools.partial(jnp.dot, preferred_element_type=f32)

    square = (state_rows, state_rows)
    named = slot_ref[...] == iota(square, 0)
    adapter = jnp.sum(jnp.where(named, iota(square, 1), 0).astype(f32), axis=1, keepdims=True)
    adapter = adapter.astype(jnp.int32)
    trained = jnp.max((act_ref[...] == adapter).astype(f32), axis=1, keepdims=True)
    place = jnp.where(ids_ref[...] == adapter, trained, 0.0).astype(bf16)
    of_chip = (iota((chips, state_rows), 1) // 4 == iota((chips, state_rows), 0)).astype(f32).astype(bf16)
    member = dot(of_chip, place)
    earlier = (iota((tokens, tokens), 0) < iota((tokens, tokens), 1)).astype(f32).astype(bf16)
    before = dot(member.astype(bf16), earlier)
    more = jnp.max(jnp.where((member > 0) & (before >= offset + slots), 1.0, 0.0))

    local = (iota((state_rows, LANES), 0) + 2 * core_ref[0]) % 4
    lane = iota((state_rows, LANES), 1)
    embed_lane, embed_row = iota((rank, LANES), 1), iota((rank, LANES), 0)
    cot_low = dot(cot_ref[...], (embed_lane == embed_row).astype(f32).astype(bf16)).astype(bf16)
    cot_high = dot(cot_ref[...], (embed_lane == embed_row + rank).astype(f32).astype(bf16)).astype(bf16)
    chosen = [
        jnp.where(before == offset + i, member, 0.0).astype(bf16) for i in range(slots)
    ]
    moved = dot(jnp.concatenate(chosen, axis=0), feat_ref[...])
    for i in range(slots):
        for b in range(blocks):
            scr[pl.ds(i * blocks + b, chips, stride=rows), :] = moved[
                i * chips : (i + 1) * chips, b * LANES : (b + 1) * LANES
            ]
    tags = jnp.where(iota((chips, LANES), 1) == 4 * slots, more, 0.0)
    for i in range(slots):
        tag = (lane == 4 * i + local).astype(f32).astype(bf16)
        of_token = lax.dot_general(place, tag, (((0,), (0,)), ((), ())), preferred_element_type=f32)
        tags = tags + dot(chosen[i], of_token.astype(bf16))
    for p in range(slots // 2):
        pair = dot(chosen[2 * p], cot_low) + dot(chosen[2 * p + 1], cot_high)
        scr[pl.ds(slots * blocks + p, chips, stride=rows), :] = pair
    for r in range(slots * blocks + slots // 2, rows):
        scr[pl.ds(r, chips, stride=rows), :] = tags
    out_ref[...] = scr[...].astype(bf16).reshape(chips, tiles, 4, LANES)


def pack(slots, offset, core, ids, slot_of, active, features, cotangent, chips):
    blocks = features.shape[1] // LANES
    rows = message_rows(slots, blocks)
    return pl.pallas_call(
        functools.partial(pack_kernel, slots, offset),
        out_shape=jax.ShapeDtypeStruct((chips, rows // 4, 4, LANES), features.dtype),
        in_specs=[SMEM, VMEM, VMEM, VMEM, VMEM, VMEM],
        out_specs=VMEM,
        scratch_shapes=[pltpu.VMEM((chips * rows, LANES), jnp.float32)],
        name=f"pack{slots}",
    )(core, ids, slot_of, active, features, cotangent)


def grad_kernel(slots, in_ref, own_ref, other_ref, flag_ref, scr):
    chips, tiles = in_ref.shape[0], in_ref.shape[1]
    rows = tiles * 4
    half, columns = own_ref.shape
    rank = half // 2
    blocks = columns // LANES
    f32, bf16 = jnp.float32, jnp.bfloat16
    scr[...] = in_ref[...].reshape(chips * rows, LANES).astype(f32)
    low = iota((chips, LANES), 1) < rank
    tags = scr[pl.ds(rows - 1, chips, stride=rows), :]
    weights, wide = [], []
    for i in range(slots):
        pair = scr[pl.ds(slots * blocks + i // 2, chips, stride=rows), :]
        one = jnp.where(low if i % 2 == 0 else ~low, pair, 0.0)
        both = one + pltpu.roll(one, rank, 1)
        h = [tags[:, 4 * i + l : 4 * i + l + 1] for l in range(4)]
        weights.append(
            jnp.concatenate(
                [both * jnp.where(low, h[0], h[1]), both * jnp.where(low, h[2], h[3])], axis=1
            ).astype(bf16)
        )
        wide.append(
            jnp.concatenate(
                [scr[pl.ds(i * blocks + b, chips, stride=rows), :] for b in range(blocks)], axis=1
            ).astype(bf16)
        )
    total = lax.dot_general(
        jnp.concatenate(weights, axis=0),
        jnp.concatenate(wide, axis=0),
        (((0,), (0,)), ((), ())),
        preferred_element_type=f32,
    )
    own_ref[...] = total[:half]
    other_ref[:half, :] = total[half:]
    more = jnp.max(tags[:, 4 * slots : 4 * slots + 1])
    other_ref[half:, :] = jnp.full((8, columns), more, f32)
    flag_ref[...] = jnp.full(flag_ref.shape, more, f32)


def partial_gradients(slots, received, half, columns):
    chips, tiles = received.shape[0], received.shape[1]
    f32 = jnp.float32
    return pl.pallas_call(
        functools.partial(grad_kernel, slots),
        out_shape=(
            jax.ShapeDtypeStruct((half, columns), f32),
            jax.ShapeDtypeStruct((half + 8, columns), f32),
            jax.ShapeDtypeStruct((8, LANES), f32),
        ),
        in_specs=[VMEM],
        out_specs=(VMEM, VMEM, VMEM),
        scratch_shapes=[pltpu.VMEM((chips * tiles * 4, LANES), f32)],
        name=f"grad{slots}",
    )(received)


def adam_kernel(
    own_index_ref,
    one_ref,
    two_ref,
    slot_ref,
    act_ref,
    own_ref,
    other_ref,
    extra_ref,
    weight_ref,
    mc_ref,
    ms_ref,
    vc_ref,
    vs_ref,
    dir_ref,
    mc_out,
    ms_out,
    vc_out,
    vs_out,
    served_ref,
):
    f32, bf16 = jnp.float32, jnp.bfloat16
    held, rank, columns = weight_ref.shape
    pairs = rank // 2
    spread = iota((rank, pairs), 0) // 2 == iota((rank, pairs), 1)

    def per_row(scales):
        return jnp.sum(jnp.where(spread, scales, 0.0), axis=1, keepdims=True)

    def per_pair(values):
        return jnp.max(jnp.where(spread, values, 0.0), axis=0, keepdims=True)

    for j in range(held):
        state_row = own_index_ref[0] * held + j
        adapter = jnp.max(jnp.where(slot_ref[...] == state_row, iota(slot_ref.shape, 1), -1).astype(f32))
        keep = jnp.max((act_ref[...].astype(f32) == adapter).astype(f32)) > 0
        at = slice(j * rank, (j + 1) * rank)
        gradient = own_ref[at, :] + other_ref[at, :] + extra_ref[at, :]
        m_code, v_code, weight = mc_ref[j], vc_ref[j], weight_ref[j]
        m_scale, v_scale = ms_ref[j : j + 1, :], vs_ref[j : j + 1, :]
        moment = beta_one * (m_code.astype(f32) * per_row(m_scale)) + (1.0 - beta_one) * gradient
        second = beta_two * (v_code.astype(f32) * per_row(v_scale)) + (1.0 - beta_two) * gradient * gradient
        direction = (moment / one_ref[j]) / (jnp.sqrt(second / two_ref[j]) + adam_eps)
        m_new = per_pair(jnp.max(jnp.abs(moment), axis=1, keepdims=True)) + scale_eps
        v_new = per_pair(jnp.max(second, axis=1, keepdims=True)) + scale_eps
        weight_f = weight.astype(f32)
        served = (weight_f - learn_rate * (direction + decay_rate * weight_f)).astype(bf16)
        dir_ref[j] = jnp.where(keep, direction, 0.0)
        mc_out[j] = jnp.where(keep, moment / per_row(m_new), m_code.astype(f32)).astype(bf16)
        vc_out[j] = jnp.where(keep, second / per_row(v_new), v_code.astype(f32)).astype(bf16)
        ms_out[j : j + 1, :] = jnp.where(keep, m_new, m_scale)
        vs_out[j : j + 1, :] = jnp.where(keep, v_new, v_scale)
        served_ref[j] = jnp.where(keep, served.astype(f32), weight_f).astype(bf16)


def adam(own_index, one, two, slot_of, active, own, other, extra, weight, m_code, m_scale, v_code, v_scale):
    f32 = jnp.float32
    like = jax.ShapeDtypeStruct
    return pl.pallas_call(
        adam_kernel,
        out_shape=(
            like(weight.shape, f32),
            like(m_code.shape, m_code.dtype),
            like(m_scale.shape, f32),
            like(v_code.shape, v_code.dtype),
            like(v_scale.shape, f32),
            like(weight.shape, weight.dtype),
        ),
        in_specs=[SMEM, SMEM, SMEM] + [VMEM] * 10,
        out_specs=(VMEM,) * 6,
        name="adam",
    )(own_index, one, two, slot_of, active, own, other, extra, weight, m_code, m_scale, v_code, v_scale)


def on_device(
    features, cotangent, adapter_ids, slot_of, active_ids, step_counts,
    weight, m_code, m_scale, v_code, v_scale,
):
    columns = features.shape[1]
    held, rank = weight.shape[0], weight.shape[1]
    half = held * rank
    chips = lax.axis_size(("x", "z"))
    core = lax.axis_index("core").astype(jnp.int32).reshape(1)
    owner = lax.axis_index(("x", "z", "core")).astype(jnp.int32).reshape(1)
    ids = adapter_ids.reshape(1, -1)
    slots_row = slot_of.reshape(1, -1)
    active = active_ids.reshape(1, -1)
    count = (step_counts + 1).astype(jnp.float32)
    one = 1.0 - jnp.power(beta_one, count)
    two = 1.0 - jnp.power(beta_two, count)
    swap = [(0, 1), (1, 0)]

    def exchange(slots, offset):
        sent = pack(slots, offset, core, ids, slots_row, active, features, cotangent, chips)
        received = lax.all_to_all(sent, ("x", "z"), split_axis=0, concat_axis=0, tiled=True)
        own, other, flag = partial_gradients(slots, received, half, columns)
        return own, lax.ppermute(other, "core", swap), flag

    own, other, flag = exchange(FIRST, 0)
    overflow = flag[0, 0] + other[half, 0] > 0

    def rest():
        more, yet, _ = exchange(8 - FIRST, FIRST)
        return more + yet[:half]

    extra = lax.cond(overflow, rest, lambda: jnp.zeros((half, columns), jnp.float32))
    direction, m_new, ms_new, v_new, vs_new, served = adam(
        owner, one, two, slots_row, active, own, other, extra,
        weight, m_code, m_scale.reshape(held, -1), v_code, v_scale.reshape(held, -1),
    )
    copies = jnp.broadcast_to(served, (lax.axis_size("replica"), *served.shape))
    parts = lax.all_to_all(copies, "replica", split_axis=0, concat_axis=0, tiled=True)
    served = jnp.moveaxis(parts, 0, 2).reshape(held, rank, -1)
    return (
        direction, m_new, ms_new.reshape(m_scale.shape), v_new, vs_new.reshape(v_scale.shape), served,
    )


def solution(mesh):
    owners, replicas = mesh.devices.shape
    fine = Mesh(mesh.devices.reshape(4, owners // 8, 2, replicas), ("x", "z", "core", "replica"))
    owner = ("x", "z", "core")
    state = P(owner, None, "replica")
    return jax.shard_map(
        on_device,
        mesh=fine,
        in_specs=(
            P(owner, "replica"), P(owner, None), P(owner, None), P(), P(), P(owner),
            state, state, state, state, state,
        ),
        out_specs=(state, state, state, state, state, P(owner, None, None)),
        check_vma=False,
    )
```

```python
import functools

import jax
import jax.numpy as jnp
from jax import lax
from jax.experimental import pallas as pl
from jax.experimental.pallas import tpu as pltpu
from jax.sharding import Mesh
from jax.sharding import PartitionSpec as P

beta_one = 0.9
beta_two = 0.999
adam_eps = 1e-08
scale_eps = 1e-06
learn_rate = 0.001
decay_rate = 0.01

LANES = 128
FIRST = 6
VMEM = pl.BlockSpec(memory_space=pltpu.VMEM)
SMEM = pl.BlockSpec(memory_space=pltpu.SMEM)
GRANT = pltpu.CompilerParams(vmem_limit_bytes=16 << 20)


def message_rows(slots, blocks):
    rows = slots * blocks + slots // 2 + 1
    return -(-rows // 4) * 4


def iota(shape, dim):
    return lax.broadcasted_iota(jnp.int32, shape, dim)


def pack_kernel(slots, offset, core_ref, ids_ref, slot_ref, act_ref, feat_ref, cot_ref, out_ref, scr):
    tokens, columns = feat_ref.shape
    rank = cot_ref.shape[0]
    state_rows = slot_ref.shape[1]
    chips, tiles = out_ref.shape[0], out_ref.shape[1]
    rows, blocks = tiles * 4, columns // LANES
    f32, bf16 = jnp.float32, jnp.bfloat16
    dot = functools.partial(jnp.dot, preferred_element_type=f32)

    square = (state_rows, state_rows)
    named = slot_ref[...] == iota(square, 0)
    adapter = jnp.sum(jnp.where(named, iota(square, 1), 0).astype(f32), axis=1, keepdims=True)
    adapter = adapter.astype(jnp.int32)
    trained = jnp.max((act_ref[...] == adapter).astype(f32), axis=1, keepdims=True)
    place = jnp.where(ids_ref[...] == adapter, trained, 0.0).astype(bf16)
    of_chip = (iota((chips, state_rows), 1) // 4 == iota((chips, state_rows), 0)).astype(f32).astype(bf16)
    member = dot(of_chip, place)
    earlier = (iota((tokens, tokens), 0) < iota((tokens, tokens), 1)).astype(f32).astype(bf16)
    before = dot(member.astype(bf16), earlier)
    late = jnp.where((member > 0) & (before >= offset + slots), 1.0, 0.0)
    more = jnp.max(jnp.max(late, axis=1, keepdims=True), axis=0, keepdims=True)

    local = (iota((state_rows, LANES), 0) + 2 * core_ref[0]) % 4
    lane = iota((state_rows, LANES), 1)
    embed_lane, embed_row = iota((rank, LANES), 1), iota((rank, LANES), 0)
    over_first = functools.partial(
        lax.dot_general, dimension_numbers=(((0,), (0,)), ((), ())), preferred_element_type=f32
    )
    low = (embed_lane == embed_row).astype(f32).astype(bf16)
    high = (embed_lane == embed_row + rank).astype(f32).astype(bf16)
    cot_low = over_first(cot_ref[...], low).astype(bf16)
    cot_high = over_first(cot_ref[...], high).astype(bf16)
    chosen = [
        jnp.where(before == offset + i, member, 0.0).astype(bf16) for i in range(slots)
    ]
    moved = dot(jnp.concatenate(chosen, axis=0), feat_ref[...])
    for i in range(slots):
        for b in range(blocks):
            scr[pl.ds(i * blocks + b, chips, stride=rows), :] = moved[
                i * chips : (i + 1) * chips, b * LANES : (b + 1) * LANES
            ]
    tags = jnp.where(iota((chips, LANES), 1) == 4 * slots, more, 0.0)
    for i in range(slots):
        tag = (lane == 4 * i + local).astype(f32).astype(bf16)
        tags = tags + dot(chosen[i], over_first(place, tag).astype(bf16))
    for p in range(slots // 2):
        pair = dot(chosen[2 * p], cot_low) + dot(chosen[2 * p + 1], cot_high)
        scr[pl.ds(slots * blocks + p, chips, stride=rows), :] = pair
    for r in range(slots * blocks + slots // 2, rows):
        scr[pl.ds(r, chips, stride=rows), :] = tags
    out_ref[...] = scr[...].astype(bf16).reshape(chips, tiles, 4, LANES)


def pack(slots, offset, core, ids, slot_of, active, features, cotangent, chips):
    blocks = features.shape[1] // LANES
    rows = message_rows(slots, blocks)
    return pl.pallas_call(
        functools.partial(pack_kernel, slots, offset),
        out_shape=jax.ShapeDtypeStruct((chips, rows // 4, 4, LANES), features.dtype),
        in_specs=[SMEM, VMEM, VMEM, VMEM, VMEM, VMEM],
        out_specs=VMEM,
        scratch_shapes=[pltpu.VMEM((chips * rows, LANES), jnp.float32)],
        compiler_params=GRANT,
        name=f"pack{slots}",
    )(core, ids, slot_of, active, features, cotangent)


def grad_kernel(slots, in_ref, own_ref, other_ref, flag_ref, scr):
    chips, tiles = in_ref.shape[0], in_ref.shape[1]
    rows = tiles * 4
    half, columns = own_ref.shape
    rank = half // 2
    blocks = columns // LANES
    f32, bf16 = jnp.float32, jnp.bfloat16
    scr[...] = in_ref[...].reshape(chips * rows, LANES).astype(f32)
    low = iota((chips, LANES), 1) < rank
    tags = scr[pl.ds(rows - 1, chips, stride=rows), :]
    weights, wide = [], []
    for i in range(slots):
        pair = scr[pl.ds(slots * blocks + i // 2, chips, stride=rows), :]
        one = jnp.where(low if i % 2 == 0 else ~low, pair, 0.0)
        both = one + pltpu.roll(one, rank, 1)
        h = [tags[:, 4 * i + l : 4 * i + l + 1] for l in range(4)]
        weights.append(
            jnp.concatenate(
                [both * jnp.where(low, h[0], h[1]), both * jnp.where(low, h[2], h[3])], axis=1
            ).astype(bf16)
        )
        wide.append(
            jnp.concatenate(
                [scr[pl.ds(i * blocks + b, chips, stride=rows), :] for b in range(blocks)], axis=1
            ).astype(bf16)
        )
    total = lax.dot_general(
        jnp.concatenate(weights, axis=0),
        jnp.concatenate(wide, axis=0),
        (((0,), (0,)), ((), ())),
        preferred_element_type=f32,
    )
    own_ref[...] = total[:half]
    other_ref[:half, :] = total[half:]
    more = jnp.max(tags[:, 4 * slots : 4 * slots + 1], axis=0, keepdims=True)
    other_ref[half:, :] = jnp.broadcast_to(more, (8, columns))
    flag_ref[...] = jnp.broadcast_to(more, flag_ref.shape)


def partial_gradients(slots, received, half, columns):
    chips, tiles = received.shape[0], received.shape[1]
    f32 = jnp.float32
    return pl.pallas_call(
        functools.partial(grad_kernel, slots),
        out_shape=(
            jax.ShapeDtypeStruct((half, columns), f32),
            jax.ShapeDtypeStruct((half + 8, columns), f32),
            jax.ShapeDtypeStruct((8, LANES), f32),
        ),
        in_specs=[VMEM],
        out_specs=(VMEM, VMEM, VMEM),
        scratch_shapes=[pltpu.VMEM((chips * tiles * 4, LANES), f32)],
        compiler_params=GRANT,
        name=f"grad{slots}",
    )(received)


def adam_kernel(
    own_index_ref,
    count_ref,
    slot_ref,
    act_ref,
    own_ref,
    other_ref,
    flag_ref,
    weight_ref,
    mc_ref,
    ms_ref,
    vc_ref,
    vs_ref,
    dir_ref,
    mc_out,
    ms_out,
    vc_out,
    vs_out,
    served_ref,
    more_ref,
):
    f32, bf16 = jnp.float32, jnp.bfloat16
    held, rank, columns = weight_ref.shape
    pairs = rank // 2
    spread = iota((rank, pairs), 0) // 2 == iota((rank, pairs), 1)

    def per_row(scales):
        return jnp.sum(jnp.where(spread, scales, 0.0), axis=1, keepdims=True)

    def per_pair(values):
        return jnp.max(jnp.where(spread, values, 0.0), axis=0, keepdims=True)

    def correction(beta, count):
        return 1.0 - lax.fori_loop(0, count, lambda _, power: power * beta, jnp.float32(1.0))

    more_ref[...] = flag_ref[...] + other_ref[held * rank :, :LANES]
    for j in range(held):
        state_row = own_index_ref[0] * held + j
        count = count_ref[j] + 1
        adapter = jnp.where(slot_ref[...] == state_row, iota(slot_ref.shape, 1), -1).astype(f32)
        adapter = jnp.max(adapter, axis=1, keepdims=True)
        keep = (act_ref[...].astype(f32) == adapter).astype(f32)
        keep = jnp.max(keep, axis=1, keepdims=True)
        keep_row = jnp.broadcast_to(keep, (1, pairs)) > 0
        keep = jnp.broadcast_to(keep, (rank, columns)) > 0
        at = slice(j * rank, (j + 1) * rank)
        gradient = own_ref[at, :] + other_ref[at, :]
        m_code, v_code = mc_ref[j].astype(f32), vc_ref[j].astype(f32)
        weight = weight_ref[j].astype(f32)
        m_scale, v_scale = ms_ref[j : j + 1, :], vs_ref[j : j + 1, :]
        moment = beta_one * (m_code * per_row(m_scale)) + (1.0 - beta_one) * gradient
        second = beta_two * (v_code * per_row(v_scale)) + (1.0 - beta_two) * gradient * gradient
        m_hat = moment / correction(beta_one, count)
        v_hat = second / correction(beta_two, count)
        direction = m_hat / (jnp.sqrt(v_hat) + adam_eps)
        m_new = per_pair(jnp.max(jnp.abs(moment), axis=1, keepdims=True)) + scale_eps
        v_new = per_pair(jnp.max(second, axis=1, keepdims=True)) + scale_eps
        served = weight - learn_rate * (direction + decay_rate * weight)
        served = jnp.where(keep, served, weight).astype(bf16)
        dir_ref[j] = jnp.where(keep, direction, 0.0)
        mc_out[j] = jnp.where(keep, moment / per_row(m_new), m_code).astype(bf16)
        vc_out[j] = jnp.where(keep, second / per_row(v_new), v_code).astype(bf16)
        ms_out[j : j + 1, :] = jnp.where(keep_row, m_new, m_scale)
        vs_out[j : j + 1, :] = jnp.where(keep_row, v_new, v_scale)
        for r in range(served_ref.shape[0]):
            served_ref[r, j] = served


def adam(replicas, own_index, counts, slot_of, active, own, other, flag, weight, m_code, m_scale, v_code, v_scale):
    f32 = jnp.float32
    like = jax.ShapeDtypeStruct
    return pl.pallas_call(
        adam_kernel,
        out_shape=(
            like(weight.shape, f32),
            like(m_code.shape, m_code.dtype),
            like(m_scale.shape, f32),
            like(v_code.shape, v_code.dtype),
            like(v_scale.shape, f32),
            like((replicas, *weight.shape), weight.dtype),
            like(flag.shape, f32),
        ),
        in_specs=[SMEM, SMEM] + [VMEM] * 10,
        out_specs=(VMEM,) * 7,
        compiler_params=GRANT,
        name="adam",
    )(own_index, counts, slot_of, active, own, other, flag, weight, m_code, m_scale, v_code, v_scale)


def on_device(
    features, cotangent, adapter_ids, slot_of, active_ids, step_counts,
    weight, m_code, m_scale, v_code, v_scale,
):
    columns = features.shape[1]
    held, rank = weight.shape[0], weight.shape[1]
    half = held * rank
    chips = lax.axis_size(("x", "z"))
    replicas = lax.axis_size("replica")
    core = lax.axis_index("core").astype(jnp.int32).reshape(1)
    owner = lax.axis_index(("x", "z", "core")).astype(jnp.int32).reshape(1)
    ids = adapter_ids.reshape(1, -1)
    slots_row = slot_of.reshape(1, -1)
    active = active_ids.reshape(1, -1)
    cot = cotangent.T
    scales = m_scale.reshape(held, -1), v_scale.reshape(held, -1)
    swap = [(0, 1), (1, 0)]

    def exchange(slots, offset, core):
        sent = pack(slots, offset, core, ids, slots_row, active, features, cot, chips)
        received = lax.all_to_all(sent, ("x", "z"), split_axis=0, concat_axis=0, tiled=True)
        own, other, flag = partial_gradients(slots, received, half, columns)
        return own, lax.ppermute(other, "core", swap), flag

    def update(own, other, flag):
        direction, m_new, ms_new, v_new, vs_new, copies, more = adam(
            replicas, owner, step_counts, slots_row, active, own, other, flag,
            weight, m_code, scales[0], v_code, scales[1],
        )
        parts = lax.all_to_all(copies, "replica", split_axis=0, concat_axis=0, tiled=True)
        served = jnp.moveaxis(parts, 0, 2).reshape(held, rank, -1)
        return more[0, 0], direction, m_new, ms_new, v_new, vs_new, served

    own, other, flag = exchange(FIRST, 0, core)

    def with_the_rest(state):
        here = core + (state[0] < 0).astype(jnp.int32)
        more, yet, none = exchange(8 - FIRST, FIRST, here)
        return update(own + more, jnp.concatenate([other[:half] + yet[:half], yet[half:]]), none)

    results = lax.while_loop(lambda state: state[0] > 0, with_the_rest, update(own, other, flag))
    _, direction, m_new, ms_new, v_new, vs_new, served = results
    return (
        direction, m_new, ms_new.reshape(m_scale.shape), v_new, vs_new.reshape(v_scale.shape), served,
    )


def solution(mesh):
    owners, replicas = mesh.devices.shape
    fine = Mesh(mesh.devices.reshape(4, owners // 8, 2, replicas), ("x", "z", "core", "replica"))
    owner = ("x", "z", "core")
    state = P(owner, None, "replica")
    return jax.shard_map(
        on_device,
        mesh=fine,
        in_specs=(
            P(owner, "replica"), P(owner, None), P(owner, None), P(), P(), P(owner),
            state, state, state, state, state,
        ),
        out_specs=(state, state, state, state, state, P(owner, None, None)),
        check_vma=False,
    )
```

```python
import functools

import jax
import jax.numpy as jnp
from jax import lax
from jax.experimental import pallas as pl
from jax.experimental.pallas import tpu as pltpu
from jax.sharding import Mesh
from jax.sharding import PartitionSpec as P

beta_one = 0.9
beta_two = 0.999
adam_eps = 1e-08
scale_eps = 1e-06
learn_rate = 0.001
decay_rate = 0.01

LANES = 128
FIRST = 6
VMEM = pl.BlockSpec(memory_space=pltpu.VMEM)
SMEM = pl.BlockSpec(memory_space=pltpu.SMEM)
GRANT = pltpu.CompilerParams(vmem_limit_bytes=16 << 20)


def message_rows(slots, blocks):
    rows = slots * blocks + slots // 2 + 1
    return -(-rows // 4) * 4


def iota(shape, dim):
    return lax.broadcasted_iota(jnp.int32, shape, dim)


def pack_kernel(
    slots, offset, core_ref, owner_ref, ids_ref, slot_ref, act_ref, count_ref, ms_ref, vs_ref, feat_ref, cot_ref, out_ref, aux_ref, scr
):
    tokens, columns = feat_ref.shape
    rank = cot_ref.shape[0]
    state_rows = slot_ref.shape[1]
    chips, tiles = out_ref.shape[0], out_ref.shape[1]
    rows, blocks = tiles * 4, columns // LANES
    held, pairs = ms_ref.shape
    f32, bf16 = jnp.float32, jnp.bfloat16
    dot = functools.partial(jnp.dot, preferred_element_type=f32)
    here, owner = core_ref[0], owner_ref[0]

    square = (state_rows, state_rows)
    named = slot_ref[...] == iota(square, 0)
    adapter = jnp.sum(jnp.where(named, iota(square, 1), 0).astype(f32), axis=1, keepdims=True)
    adapter = adapter.astype(jnp.int32)
    trained = jnp.max((act_ref[...] == adapter).astype(f32), axis=1, keepdims=True)
    place = jnp.where(ids_ref[...] == adapter, trained, 0.0).astype(bf16)
    of_chip = (iota((chips, state_rows), 1) // 4 == iota((chips, state_rows), 0)).astype(f32).astype(bf16)
    member = dot(of_chip, place)
    earlier = (iota((tokens, tokens), 0) < iota((tokens, tokens), 1)).astype(f32).astype(bf16)
    before = dot(member.astype(bf16), earlier)
    late = jnp.where((member > 0) & (before >= offset + slots), 1.0, 0.0)
    more = jnp.max(jnp.max(late, axis=1, keepdims=True), axis=0, keepdims=True)

    local = (iota((state_rows, LANES), 0) + 2 * here) % 4
    tag = (iota((state_rows, LANES), 1) == rank + local).astype(f32).astype(bf16)
    embed = (iota((rank, LANES), 0) == iota((rank, LANES), 1)).astype(f32).astype(bf16)
    beside = lax.dot_general(
        jnp.concatenate([cot_ref[...], place], axis=0),
        jnp.concatenate([embed, tag], axis=0),
        (((0,), (0,)), ((), ())),
        preferred_element_type=f32,
    )
    chosen = jnp.concatenate(
        [jnp.where(before == offset + i, member, 0.0).astype(bf16) for i in range(slots)], axis=0
    )
    beside = dot(chosen, beside.astype(bf16))
    moved = dot(chosen, feat_ref[...])
    of_slot = [slice(i * chips, (i + 1) * chips) for i in range(slots)]
    for i in range(slots):
        for b in range(blocks):
            scr[pl.ds(i * blocks + b, chips, stride=rows), :] = moved[of_slot[i], b * LANES : (b + 1) * LANES]
    lane = iota((chips, LANES), 1)
    tags = jnp.where(lane == 4 * slots, more, 0.0)
    for i in range(slots):
        one = jnp.where((lane >= rank) & (lane < rank + 4), beside[of_slot[i]], 0.0)
        tags = tags + pltpu.roll(one, (LANES - rank + 4 * i) % LANES, 1)
    for p in range(slots // 2):
        pair = jnp.where(lane < rank, beside[of_slot[2 * p]], pltpu.roll(beside[of_slot[2 * p + 1]], rank, 1))
        scr[pl.ds(slots * blocks + p, chips, stride=rows), :] = pair
    for r in range(slots * blocks + slots // 2, rows):
        scr[pl.ds(r, chips, stride=rows), :] = tags
    out_ref[...] = scr[...].astype(bf16).reshape(chips, tiles, 4, LANES)

    aux_ref[...] = jnp.zeros(aux_ref.shape, f32)
    aux_ref[:held, :pairs] = ms_ref[...]
    aux_ref[held : 2 * held, :pairs] = vs_ref[...]
    count = count_ref[...] + 1
    for at, beta in ((2 * held, beta_one), (2 * held + 1, beta_two)):
        power = jnp.ones(count.shape, f32)
        for bit in range(8):
            power = jnp.where((count >> bit) % 2 == 1, power * beta ** (1 << bit), power)
        aux_ref[at : at + 1, :held] = 1.0 / (1.0 - power)
    state_row = iota((state_rows, held), 0) - held * owner
    mine = jnp.where(state_row == iota((state_rows, held), 1), trained, 0.0)
    aux_ref[2 * held + 2 : 2 * held + 3, :held] = jnp.max(mine, axis=0, keepdims=True)


def pack(slots, offset, core, owner, ids, slot_of, active, counts, m_scale, v_scale, features, cotangent, chips):
    blocks = features.shape[1] // LANES
    rows = message_rows(slots, blocks)
    return pl.pallas_call(
        functools.partial(pack_kernel, slots, offset),
        out_shape=(
            jax.ShapeDtypeStruct((chips, rows // 4, 4, LANES), features.dtype),
            jax.ShapeDtypeStruct((8, LANES), jnp.float32),
        ),
        in_specs=[SMEM, SMEM] + [VMEM] * 8,
        out_specs=(VMEM, VMEM),
        scratch_shapes=[pltpu.VMEM((chips * rows, LANES), jnp.float32)],
        compiler_params=GRANT,
        name=f"pack{slots}",
    )(core, owner, ids, slot_of, active, counts, m_scale, v_scale, features, cotangent)


def grad_kernel(slots, in_ref, own_ref, other_ref, flag_ref, scr):
    chips, tiles = in_ref.shape[0], in_ref.shape[1]
    rows = tiles * 4
    half, columns = own_ref.shape
    rank = half // 2
    blocks = columns // LANES
    f32, bf16 = jnp.float32, jnp.bfloat16
    scr[...] = in_ref[...].reshape(chips * rows, LANES).astype(f32)
    low = iota((chips, LANES), 1) < rank
    tags = scr[pl.ds(rows - 1, chips, stride=rows), :]
    weights, wide = [], []
    for i in range(slots):
        pair = scr[pl.ds(slots * blocks + i // 2, chips, stride=rows), :]
        one = jnp.where(low if i % 2 == 0 else ~low, pair, 0.0)
        both = one + pltpu.roll(one, rank, 1)
        h = [tags[:, 4 * i + l : 4 * i + l + 1] for l in range(4)]
        weights.append(
            jnp.concatenate(
                [both * jnp.where(low, h[0], h[1]), both * jnp.where(low, h[2], h[3])], axis=1
            ).astype(bf16)
        )
        wide.append(
            jnp.concatenate(
                [scr[pl.ds(i * blocks + b, chips, stride=rows), :] for b in range(blocks)], axis=1
            ).astype(bf16)
        )
    total = lax.dot_general(
        jnp.concatenate(weights, axis=0),
        jnp.concatenate(wide, axis=0),
        (((0,), (0,)), ((), ())),
        preferred_element_type=f32,
    )
    own_ref[...] = total[:half]
    other_ref[:half, :] = total[half:]
    more = jnp.max(tags[:, 4 * slots : 4 * slots + 1], axis=0, keepdims=True)
    other_ref[half:, :] = jnp.broadcast_to(more, (8, columns))
    flag_ref[...] = jnp.broadcast_to(more, flag_ref.shape)


def partial_gradients(slots, received, half, columns):
    chips, tiles = received.shape[0], received.shape[1]
    f32 = jnp.float32
    return pl.pallas_call(
        functools.partial(grad_kernel, slots),
        out_shape=(
            jax.ShapeDtypeStruct((half, columns), f32),
            jax.ShapeDtypeStruct((half + 8, columns), f32),
            jax.ShapeDtypeStruct((8, LANES), f32),
        ),
        in_specs=[VMEM],
        out_specs=(VMEM, VMEM, VMEM),
        scratch_shapes=[pltpu.VMEM((chips * tiles * 4, LANES), f32)],
        compiler_params=GRANT,
        name=f"grad{slots}",
    )(received)


def moments(j, aux_ref, own_ref, other_ref, mc_ref, vc_ref, spread):
    f32 = jnp.float32
    held, rank, _ = mc_ref.shape
    pairs = rank // 2

    def per_row(at):
        return jnp.sum(jnp.where(spread, aux_ref[at : at + 1, :pairs], 0.0), axis=1, keepdims=True)

    at = slice(j * rank, (j + 1) * rank)
    gradient = own_ref[at, :] + other_ref[at, :]
    moment = mc_ref[j].astype(f32) * (beta_one * per_row(j)) + (1.0 - beta_one) * gradient
    second = vc_ref[j].astype(f32) * (beta_two * per_row(held + j)) + (1.0 - beta_two) * gradient * gradient
    inverse_one = aux_ref[2 * held : 2 * held + 1, j : j + 1]
    inverse_two = aux_ref[2 * held + 1 : 2 * held + 2, j : j + 1]
    direction = (moment * inverse_one) / (jnp.sqrt(second * inverse_two) + adam_eps)
    return moment, second, direction


def row_spread(rank):
    return iota((rank, rank // 2), 0) // 2 == iota((rank, rank // 2), 1)


def trained_row(aux_ref, held, j, shape):
    return jnp.broadcast_to(aux_ref[2 * held + 2 : 2 * held + 3, j : j + 1], shape) > 0


def serve_kernel(aux_ref, own_ref, other_ref, weight_ref, mc_ref, vc_ref, served_ref):
    held, rank, columns = weight_ref.shape
    spread = row_spread(rank)
    for j in range(held):
        _, _, direction = moments(j, aux_ref, own_ref, other_ref, mc_ref, vc_ref, spread)
        weight = weight_ref[j].astype(jnp.float32)
        served = weight - learn_rate * (direction + decay_rate * weight)
        served = jnp.where(trained_row(aux_ref, held, j, weight.shape), served, weight)
        served = served.astype(served_ref.dtype)
        for r in range(served_ref.shape[0]):
            served_ref[r, j] = served


def serve(replicas, aux, own, other, weight, m_code, v_code):
    return pl.pallas_call(
        serve_kernel,
        out_shape=jax.ShapeDtypeStruct((replicas, *weight.shape), weight.dtype),
        in_specs=[VMEM] * 6,
        out_specs=VMEM,
        compiler_params=GRANT,
        name="serve",
    )(aux, own, other, weight, m_code, v_code)


def state_kernel(
    aux_ref, own_ref, other_ref, flag_ref, mc_ref, vc_ref, dir_ref, mc_out, ms_out, vc_out, vs_out, more_ref
):
    f32 = jnp.float32
    held, rank, columns = mc_ref.shape
    pairs = rank // 2
    spread = row_spread(rank)

    def per_pair(values):
        return jnp.max(jnp.where(spread, values, 0.0), axis=0, keepdims=True)

    def per_row(scales):
        return jnp.sum(jnp.where(spread, scales, 0.0), axis=1, keepdims=True)

    more_ref[...] = flag_ref[...] + other_ref[held * rank :, :LANES]
    for j in range(held):
        moment, second, direction = moments(j, aux_ref, own_ref, other_ref, mc_ref, vc_ref, spread)
        keep = trained_row(aux_ref, held, j, moment.shape)
        keep_row = trained_row(aux_ref, held, j, (1, pairs))
        m_new = per_pair(jnp.max(jnp.abs(moment), axis=1, keepdims=True)) + scale_eps
        v_new = per_pair(jnp.max(second, axis=1, keepdims=True)) + scale_eps
        dir_ref[j] = jnp.where(keep, direction, 0.0)
        m_code, v_code = moment / per_row(m_new), second / per_row(v_new)
        mc_out[j] = jnp.where(keep, m_code, mc_ref[j].astype(f32)).astype(mc_out.dtype)
        vc_out[j] = jnp.where(keep, v_code, vc_ref[j].astype(f32)).astype(vc_out.dtype)
        ms_out[j : j + 1, :] = jnp.where(keep_row, m_new, aux_ref[j : j + 1, :pairs])
        vs_out[j : j + 1, :] = jnp.where(keep_row, v_new, aux_ref[held + j : held + j + 1, :pairs])


def state(aux, own, other, flag, m_code, v_code):
    f32 = jnp.float32
    like = jax.ShapeDtypeStruct
    scales = like((m_code.shape[0], m_code.shape[1] // 2), f32)
    return pl.pallas_call(
        state_kernel,
        out_shape=(
            like(m_code.shape, f32),
            like(m_code.shape, m_code.dtype),
            scales,
            like(v_code.shape, v_code.dtype),
            scales,
            like(flag.shape, f32),
        ),
        in_specs=[VMEM] * 6,
        out_specs=(VMEM,) * 6,
        compiler_params=GRANT,
        name="state",
    )(aux, own, other, flag, m_code, v_code)


def on_device(
    features, cotangent, adapter_ids, slot_of, active_ids, step_counts,
    weight, m_code, m_scale, v_code, v_scale,
):
    columns = features.shape[1]
    held, rank = weight.shape[0], weight.shape[1]
    half = held * rank
    chips = lax.axis_size(("x", "z"))
    replicas = lax.axis_size("replica")
    core = lax.axis_index("core").astype(jnp.int32).reshape(1)
    owner = lax.axis_index(("x", "z", "core")).astype(jnp.int32).reshape(1)
    small = (
        adapter_ids.reshape(1, -1), slot_of.reshape(1, -1), active_ids.reshape(1, -1), step_counts.reshape(1, -1),
        m_scale.reshape(held, -1), v_scale.reshape(held, -1),
    )
    swap = [(0, 1), (1, 0)]

    def exchange(slots, offset, core):
        sent, aux = pack(slots, offset, core, owner, *small, features, cotangent.T, chips)
        received = lax.all_to_all(sent, ("x", "z"), split_axis=0, concat_axis=0, tiled=True)
        own, other, flag = partial_gradients(slots, received, half, columns)
        return own, lax.ppermute(other, "core", swap), flag, aux

    def update(own, other, flag, aux):
        copies = serve(replicas, aux, own, other, weight, m_code, v_code)
        parts = lax.all_to_all(copies, "replica", split_axis=0, concat_axis=0, tiled=True)
        served = jnp.moveaxis(parts, 0, 2).reshape(held, rank, -1)
        direction, m_new, ms_new, v_new, vs_new, more = state(aux, own, other, flag, m_code, v_code)
        return more[0, 0], direction, m_new, ms_new, v_new, vs_new, served

    own, other, flag, aux = exchange(FIRST, 0, core)

    def with_the_rest(carry):
        here = core + (carry[0] < 0).astype(jnp.int32)
        more, yet, none, again = exchange(8 - FIRST, FIRST, here)
        return update(own + more, jnp.concatenate([other[:half] + yet[:half], yet[half:]]), none, again)

    results = lax.while_loop(lambda carry: carry[0] > 0, with_the_rest, update(own, other, flag, aux))
    _, direction, m_new, ms_new, v_new, vs_new, served = results
    return (
        direction, m_new, ms_new.reshape(m_scale.shape), v_new, vs_new.reshape(v_scale.shape), served,
    )


def solution(mesh):
    owners, replicas = mesh.devices.shape
    fine = Mesh(mesh.devices.reshape(4, owners // 8, 2, replicas), ("x", "z", "core", "replica"))
    owner = ("x", "z", "core")
    block = P(owner, None, "replica")
    return jax.shard_map(
        on_device,
        mesh=fine,
        in_specs=(
            P(owner, "replica"), P(owner, None), P(owner, None), P(), P(), P(owner),
            block, block, block, block, block,
        ),
        out_specs=(block, block, block, block, block, P(owner, None, None)),
        check_vma=False,
    )
```

```python
import functools

import jax
import jax.numpy as jnp
from jax import lax
from jax.experimental import pallas as pl
from jax.experimental.pallas import tpu as pltpu
from jax.sharding import Mesh
from jax.sharding import PartitionSpec as P

beta_one = 0.9
beta_two = 0.999
adam_eps = 1e-08
scale_eps = 1e-06
learn_rate = 0.001
decay_rate = 0.01

LANES = 128
FIRST = 6
VMEM = pl.BlockSpec(memory_space=pltpu.VMEM)
SMEM = pl.BlockSpec(memory_space=pltpu.SMEM)
ANY = pl.BlockSpec(memory_space=pl.ANY)
GRANT = pltpu.CompilerParams(vmem_limit_bytes=16 << 20)


def message_rows(slots, blocks):
    rows = slots * blocks + slots // 2 + 1
    return -(-rows // 4) * 4


def iota(shape, dim):
    return lax.broadcasted_iota(jnp.int32, shape, dim)


def pack_kernel(
    slots, offset, core_ref, owner_ref, ids_ref, slot_ref, act_ref, count_ref, ms_ref, vs_ref, feat_hbm, cot_ref,
    out_ref, aux_ref, scr, feat_ref, feat_sem,
):
    tokens, columns = feat_ref.shape
    rank = cot_ref.shape[0]
    state_rows = slot_ref.shape[1]
    chips, tiles = out_ref.shape[0], out_ref.shape[1]
    rows, blocks = tiles * 4, columns // LANES
    held, pairs = ms_ref.shape
    f32, bf16 = jnp.float32, jnp.bfloat16
    dot = functools.partial(jnp.dot, preferred_element_type=f32)
    here, owner = core_ref[0], owner_ref[0]
    fetch = pltpu.make_async_copy(feat_hbm, feat_ref, feat_sem)
    fetch.start()

    square = (state_rows, state_rows)
    named = slot_ref[...] == iota(square, 0)
    adapter = jnp.sum(jnp.where(named, iota(square, 1), 0).astype(f32), axis=1, keepdims=True)
    adapter = adapter.astype(jnp.int32)
    trained = jnp.max((act_ref[...] == adapter).astype(f32), axis=1, keepdims=True)
    place = jnp.where(ids_ref[...] == adapter, trained, 0.0).astype(bf16)
    of_chip = (iota((chips, state_rows), 1) // 4 == iota((chips, state_rows), 0)).astype(f32).astype(bf16)
    member = dot(of_chip, place)
    earlier = (iota((tokens, tokens), 0) < iota((tokens, tokens), 1)).astype(f32).astype(bf16)
    before = dot(member.astype(bf16), earlier)
    late = jnp.where((member > 0) & (before >= offset + slots), 1.0, 0.0)
    more = jnp.max(jnp.max(late, axis=1, keepdims=True), axis=0, keepdims=True)

    local = (iota((state_rows, LANES), 0) + 2 * here) % 4
    tag = (iota((state_rows, LANES), 1) == rank + local).astype(f32).astype(bf16)
    embed = (iota((rank, LANES), 0) == iota((rank, LANES), 1)).astype(f32).astype(bf16)
    beside = lax.dot_general(
        jnp.concatenate([cot_ref[...], place], axis=0),
        jnp.concatenate([embed, tag], axis=0),
        (((0,), (0,)), ((), ())),
        preferred_element_type=f32,
    )
    chosen = jnp.concatenate(
        [jnp.where(before == offset + i, member, 0.0).astype(bf16) for i in range(slots)], axis=0
    )
    beside = dot(chosen, beside.astype(bf16))
    fetch.wait()
    moved = dot(chosen, feat_ref[...])
    of_slot = [slice(i * chips, (i + 1) * chips) for i in range(slots)]
    for i in range(slots):
        for b in range(blocks):
            scr[pl.ds(i * blocks + b, chips, stride=rows), :] = moved[of_slot[i], b * LANES : (b + 1) * LANES]
    lane = iota((chips, LANES), 1)
    tags = jnp.where(lane == 4 * slots, more, 0.0)
    for i in range(slots):
        one = jnp.where((lane >= rank) & (lane < rank + 4), beside[of_slot[i]], 0.0)
        tags = tags + pltpu.roll(one, (LANES - rank + 4 * i) % LANES, 1)
    for p in range(slots // 2):
        pair = jnp.where(lane < rank, beside[of_slot[2 * p]], pltpu.roll(beside[of_slot[2 * p + 1]], rank, 1))
        scr[pl.ds(slots * blocks + p, chips, stride=rows), :] = pair
    for r in range(slots * blocks + slots // 2, rows):
        scr[pl.ds(r, chips, stride=rows), :] = tags
    out_ref[...] = scr[...].astype(bf16).reshape(chips, tiles, 4, LANES)

    aux_ref[...] = jnp.zeros(aux_ref.shape, f32)
    aux_ref[:held, :pairs] = ms_ref[...]
    aux_ref[held : 2 * held, :pairs] = vs_ref[...]
    count = count_ref[...] + 1
    for at, beta in ((2 * held, beta_one), (2 * held + 1, beta_two)):
        power = jnp.ones(count.shape, f32)
        for bit in range(8):
            power = jnp.where((count >> bit) % 2 == 1, power * beta ** (1 << bit), power)
        aux_ref[at : at + 1, :held] = 1.0 / (1.0 - power)
    state_row = iota((state_rows, held), 0) - held * owner
    mine = jnp.where(state_row == iota((state_rows, held), 1), trained, 0.0)
    aux_ref[2 * held + 2 : 2 * held + 3, :held] = jnp.max(mine, axis=0, keepdims=True)


def pack(slots, offset, core, owner, ids, slot_of, active, counts, m_scale, v_scale, features, cotangent, chips):
    blocks = features.shape[1] // LANES
    rows = message_rows(slots, blocks)
    return pl.pallas_call(
        functools.partial(pack_kernel, slots, offset),
        out_shape=(
            jax.ShapeDtypeStruct((chips, rows // 4, 4, LANES), features.dtype),
            jax.ShapeDtypeStruct((8, LANES), jnp.float32),
        ),
        in_specs=[SMEM, SMEM] + [VMEM] * 6 + [ANY, VMEM],
        out_specs=(VMEM, VMEM),
        scratch_shapes=[
            pltpu.VMEM((chips * rows, LANES), jnp.float32),
            pltpu.VMEM(features.shape, features.dtype),
            pltpu.SemaphoreType.DMA,
        ],
        compiler_params=GRANT,
        name=f"pack{slots}",
    )(core, owner, ids, slot_of, active, counts, m_scale, v_scale, features, cotangent)


def grad_kernel(slots, in_ref, own_ref, other_ref, flag_ref, scr):
    chips, tiles = in_ref.shape[0], in_ref.shape[1]
    rows = tiles * 4
    half, columns = own_ref.shape
    rank = half // 2
    blocks = columns // LANES
    f32, bf16 = jnp.float32, jnp.bfloat16
    scr[...] = in_ref[...].reshape(chips * rows, LANES).astype(f32)
    low = iota((chips, LANES), 1) < rank
    tags = scr[pl.ds(rows - 1, chips, stride=rows), :]
    weights, wide = [], []
    for i in range(slots):
        pair = scr[pl.ds(slots * blocks + i // 2, chips, stride=rows), :]
        one = jnp.where(low if i % 2 == 0 else ~low, pair, 0.0)
        both = one + pltpu.roll(one, rank, 1)
        h = [tags[:, 4 * i + l : 4 * i + l + 1] for l in range(4)]
        weights.append(
            jnp.concatenate(
                [both * jnp.where(low, h[0], h[1]), both * jnp.where(low, h[2], h[3])], axis=1
            ).astype(bf16)
        )
        wide.append(
            jnp.concatenate(
                [scr[pl.ds(i * blocks + b, chips, stride=rows), :] for b in range(blocks)], axis=1
            ).astype(bf16)
        )
    total = lax.dot_general(
        jnp.concatenate(weights, axis=0),
        jnp.concatenate(wide, axis=0),
        (((0,), (0,)), ((), ())),
        preferred_element_type=f32,
    )
    own_ref[...] = total[:half]
    other_ref[:half, :] = total[half:]
    more = jnp.max(tags[:, 4 * slots : 4 * slots + 1], axis=0, keepdims=True)
    other_ref[half:, :] = jnp.broadcast_to(more, (8, columns))
    flag_ref[...] = jnp.broadcast_to(more, flag_ref.shape)


def partial_gradients(slots, received, half, columns):
    chips, tiles = received.shape[0], received.shape[1]
    f32 = jnp.float32
    return pl.pallas_call(
        functools.partial(grad_kernel, slots),
        out_shape=(
            jax.ShapeDtypeStruct((half, columns), f32),
            jax.ShapeDtypeStruct((half + 8, columns), f32),
            jax.ShapeDtypeStruct((8, LANES), f32),
        ),
        in_specs=[VMEM],
        out_specs=(VMEM, VMEM, VMEM),
        scratch_shapes=[pltpu.VMEM((chips * tiles * 4, LANES), f32)],
        compiler_params=GRANT,
        name=f"grad{slots}",
    )(received)


def moments(j, aux_ref, gradient, mc_ref, vc_ref, spread):
    f32 = jnp.float32
    held, rank, _ = mc_ref.shape
    pairs = rank // 2

    def per_row(at):
        return jnp.sum(jnp.where(spread, aux_ref[at : at + 1, :pairs], 0.0), axis=1, keepdims=True)

    moment = mc_ref[j].astype(f32) * (beta_one * per_row(j)) + (1.0 - beta_one) * gradient
    second = vc_ref[j].astype(f32) * (beta_two * per_row(held + j)) + (1.0 - beta_two) * gradient * gradient
    inverse_one = aux_ref[2 * held : 2 * held + 1, j : j + 1]
    inverse_two = aux_ref[2 * held + 1 : 2 * held + 2, j : j + 1]
    direction = (moment * inverse_one) / (jnp.sqrt(second * inverse_two) + adam_eps)
    return moment, second, direction


def row_spread(rank):
    return iota((rank, rank // 2), 0) // 2 == iota((rank, rank // 2), 1)


def trained_row(aux_ref, held, j, shape):
    return jnp.broadcast_to(aux_ref[2 * held + 2 : 2 * held + 3, j : j + 1], shape) > 0


def serve_kernel(
    aux_ref, own_ref, other_hbm, weight_ref, mc_ref, vc_ref, served_hbm, other_ref, out_ref, in_sems, out_sems
):
    held, rank, columns = weight_ref.shape
    spread = row_spread(rank)
    fetches = [
        pltpu.make_async_copy(other_hbm.at[pl.ds(j * rank, rank)], other_ref.at[j], in_sems.at[j]) for j in range(held)
    ]
    for fetch in fetches:
        fetch.start()
    sends = []
    for j in range(held):
        fetches[j].wait()
        gradient = own_ref[j * rank : (j + 1) * rank, :] + other_ref[j]
        _, _, direction = moments(j, aux_ref, gradient, mc_ref, vc_ref, spread)
        weight = weight_ref[j].astype(jnp.float32)
        served = weight - learn_rate * (direction + decay_rate * weight)
        served = jnp.where(trained_row(aux_ref, held, j, weight.shape), served, weight)
        out_ref[j] = served.astype(out_ref.dtype)
        for r in range(served_hbm.shape[0]):
            send = pltpu.make_async_copy(out_ref.at[j], served_hbm.at[r, j], out_sems.at[j, r])
            send.start()
            sends.append(send)
    for send in sends:
        send.wait()


def serve(replicas, aux, own, other, weight, m_code, v_code):
    held, rank, columns = weight.shape
    return pl.pallas_call(
        serve_kernel,
        out_shape=jax.ShapeDtypeStruct((replicas, *weight.shape), weight.dtype),
        in_specs=[VMEM, VMEM, ANY, VMEM, VMEM, VMEM],
        out_specs=ANY,
        scratch_shapes=[
            pltpu.VMEM((held, rank, columns), jnp.float32),
            pltpu.VMEM(weight.shape, weight.dtype),
            pltpu.SemaphoreType.DMA((held,)),
            pltpu.SemaphoreType.DMA((held, replicas)),
        ],
        compiler_params=GRANT,
        name="serve",
    )(aux, own, other, weight, m_code, v_code)


def state_kernel(
    aux_ref, own_ref, other_ref, flag_ref, mc_ref, vc_ref, dir_ref, mc_out, ms_out, vc_out, vs_out, more_ref
):
    f32 = jnp.float32
    held, rank, columns = mc_ref.shape
    pairs = rank // 2
    spread = row_spread(rank)

    def per_pair(values):
        return jnp.max(jnp.where(spread, values, 0.0), axis=0, keepdims=True)

    def per_row(scales):
        return jnp.sum(jnp.where(spread, scales, 0.0), axis=1, keepdims=True)

    more_ref[...] = flag_ref[...] + other_ref[held * rank :, :LANES]
    for j in range(held):
        at = slice(j * rank, (j + 1) * rank)
        gradient = own_ref[at, :] + other_ref[at, :]
        moment, second, direction = moments(j, aux_ref, gradient, mc_ref, vc_ref, spread)
        keep = trained_row(aux_ref, held, j, moment.shape)
        keep_row = trained_row(aux_ref, held, j, (1, pairs))
        m_new = per_pair(jnp.max(jnp.abs(moment), axis=1, keepdims=True)) + scale_eps
        v_new = per_pair(jnp.max(second, axis=1, keepdims=True)) + scale_eps
        dir_ref[j] = jnp.where(keep, direction, 0.0)
        m_code, v_code = moment / per_row(m_new), second / per_row(v_new)
        mc_out[j] = jnp.where(keep, m_code, mc_ref[j].astype(f32)).astype(mc_out.dtype)
        vc_out[j] = jnp.where(keep, v_code, vc_ref[j].astype(f32)).astype(vc_out.dtype)
        ms_out[j : j + 1, :] = jnp.where(keep_row, m_new, aux_ref[j : j + 1, :pairs])
        vs_out[j : j + 1, :] = jnp.where(keep_row, v_new, aux_ref[held + j : held + j + 1, :pairs])


def state(aux, own, other, flag, m_code, v_code):
    f32 = jnp.float32
    like = jax.ShapeDtypeStruct
    scales = like((m_code.shape[0], m_code.shape[1] // 2), f32)
    return pl.pallas_call(
        state_kernel,
        out_shape=(
            like(m_code.shape, f32),
            like(m_code.shape, m_code.dtype),
            scales,
            like(v_code.shape, v_code.dtype),
            scales,
            like(flag.shape, f32),
        ),
        in_specs=[VMEM] * 6,
        out_specs=(VMEM,) * 6,
        compiler_params=GRANT,
        name="state",
    )(aux, own, other, flag, m_code, v_code)


def on_device(
    features, cotangent, adapter_ids, slot_of, active_ids, step_counts,
    weight, m_code, m_scale, v_code, v_scale,
):
    columns = features.shape[1]
    held, rank = weight.shape[0], weight.shape[1]
    half = held * rank
    chips = lax.axis_size(("x", "z"))
    replicas = lax.axis_size("replica")
    core = lax.axis_index("core").astype(jnp.int32).reshape(1)
    owner = lax.axis_index(("x", "z", "core")).astype(jnp.int32).reshape(1)
    small = (
        adapter_ids.reshape(1, -1), slot_of.reshape(1, -1), active_ids.reshape(1, -1), step_counts.reshape(1, -1),
        m_scale.reshape(held, -1), v_scale.reshape(held, -1),
    )
    swap = [(0, 1), (1, 0)]

    def exchange(slots, offset, core):
        sent, aux = pack(slots, offset, core, owner, *small, features, cotangent.T, chips)
        received = lax.all_to_all(sent, ("x", "z"), split_axis=0, concat_axis=0, tiled=True)
        own, other, flag = partial_gradients(slots, received, half, columns)
        return own, lax.ppermute(other, "core", swap), flag, aux

    def update(own, other, flag, aux):
        copies = serve(replicas, aux, own, other, weight, m_code, v_code)
        parts = lax.all_to_all(copies, "replica", split_axis=0, concat_axis=0, tiled=True)
        served = jnp.moveaxis(parts, 0, 2).reshape(held, rank, -1)
        direction, m_new, ms_new, v_new, vs_new, more = state(aux, own, other, flag, m_code, v_code)
        return more[0, 0], direction, m_new, ms_new, v_new, vs_new, served

    own, other, flag, aux = exchange(FIRST, 0, core)

    def with_the_rest(carry):
        here = core + (carry[0] < 0).astype(jnp.int32)
        more, yet, none, again = exchange(8 - FIRST, FIRST, here)
        return update(own + more, jnp.concatenate([other[:half] + yet[:half], yet[half:]]), none, again)

    results = lax.while_loop(lambda carry: carry[0] > 0, with_the_rest, update(own, other, flag, aux))
    _, direction, m_new, ms_new, v_new, vs_new, served = results
    return (
        direction, m_new, ms_new.reshape(m_scale.shape), v_new, vs_new.reshape(v_scale.shape), served,
    )


def solution(mesh):
    owners, replicas = mesh.devices.shape
    fine = Mesh(mesh.devices.reshape(4, owners // 8, 2, replicas), ("x", "z", "core", "replica"))
    owner = ("x", "z", "core")
    block = P(owner, None, "replica")
    return jax.shard_map(
        on_device,
        mesh=fine,
        in_specs=(
            P(owner, "replica"), P(owner, None), P(owner, None), P(), P(), P(owner),
            block, block, block, block, block,
        ),
        out_specs=(block, block, block, block, block, P(owner, None, None)),
        check_vma=False,
    )
```

```python
import functools

import jax
import jax.numpy as jnp
from jax import lax
from jax.experimental import pallas as pl
from jax.experimental.pallas import tpu as pltpu
from jax.sharding import Mesh
from jax.sharding import PartitionSpec as P

beta_one = 0.9
beta_two = 0.999
adam_eps = 1e-08
scale_eps = 1e-06
learn_rate = 0.001
decay_rate = 0.01

LANES = 128
FIRST = 6
VMEM = pl.BlockSpec(memory_space=pltpu.VMEM)
SMEM = pl.BlockSpec(memory_space=pltpu.SMEM)
ANY = pl.BlockSpec(memory_space=pl.ANY)
GRANT = pltpu.CompilerParams(vmem_limit_bytes=16 << 20)


def message_rows(slots, blocks):
    rows = slots * blocks + slots // 2 + 1
    return -(-rows // 4) * 4


def iota(shape, dim):
    return lax.broadcasted_iota(jnp.int32, shape, dim)


def pack_kernel(
    slots, offset, core_ref, owner_ref, ids_ref, slot_ref, act_ref, count_ref, ms_ref, vs_ref, feat_hbm, cot_ref,
    out_ref, aux_ref, scr, feat_ref, feat_sem,
):
    tokens, columns = feat_ref.shape
    rank = cot_ref.shape[0]
    state_rows = slot_ref.shape[1]
    chips, tiles = out_ref.shape[0], out_ref.shape[1]
    rows, blocks = tiles * 4, columns // LANES
    held, pairs = ms_ref.shape
    f32, bf16 = jnp.float32, jnp.bfloat16
    dot = functools.partial(jnp.dot, preferred_element_type=f32)
    here, owner = core_ref[0], owner_ref[0]
    fetch = pltpu.make_async_copy(feat_hbm, feat_ref, feat_sem)
    fetch.start()

    square = (state_rows, state_rows)
    named = slot_ref[...] == iota(square, 0)
    adapter = jnp.sum(jnp.where(named, iota(square, 1), 0).astype(f32), axis=1, keepdims=True)
    adapter = adapter.astype(jnp.int32)
    trained = jnp.max((act_ref[...] == adapter).astype(f32), axis=1, keepdims=True)
    place = jnp.where(ids_ref[...] == adapter, trained, 0.0).astype(bf16)
    of_chip = (iota((chips, state_rows), 1) // 4 == iota((chips, state_rows), 0)).astype(f32).astype(bf16)
    member = dot(of_chip, place)
    earlier = (iota((tokens, tokens), 0) < iota((tokens, tokens), 1)).astype(f32).astype(bf16)
    before = dot(member.astype(bf16), earlier)
    late = jnp.where((member > 0) & (before >= offset + slots), 1.0, 0.0)
    more = jnp.max(jnp.max(late, axis=1, keepdims=True), axis=0, keepdims=True)

    local = (iota((state_rows, LANES), 0) + 2 * here) % 4
    tag = (iota((state_rows, LANES), 1) == rank + local).astype(f32).astype(bf16)
    embed = (iota((rank, LANES), 0) == iota((rank, LANES), 1)).astype(f32).astype(bf16)
    beside = lax.dot_general(
        jnp.concatenate([cot_ref[...], place], axis=0),
        jnp.concatenate([embed, tag], axis=0),
        (((0,), (0,)), ((), ())),
        preferred_element_type=f32,
    )
    chosen = jnp.concatenate(
        [jnp.where(before == offset + i, member, 0.0).astype(bf16) for i in range(slots)], axis=0
    )
    beside = dot(chosen, beside.astype(bf16))
    fetch.wait()
    moved = dot(chosen, feat_ref[...])
    of_slot = [slice(i * chips, (i + 1) * chips) for i in range(slots)]
    for i in range(slots):
        for b in range(blocks):
            scr[pl.ds(i * blocks + b, chips, stride=rows), :] = moved[of_slot[i], b * LANES : (b + 1) * LANES]
    lane = iota((chips, LANES), 1)
    tags = jnp.where(lane == 4 * slots, more, 0.0)
    for i in range(slots):
        one = jnp.where((lane >= rank) & (lane < rank + 4), beside[of_slot[i]], 0.0)
        tags = tags + pltpu.roll(one, (LANES - rank + 4 * i) % LANES, 1)
    for p in range(slots // 2):
        pair = jnp.where(lane < rank, beside[of_slot[2 * p]], pltpu.roll(beside[of_slot[2 * p + 1]], rank, 1))
        scr[pl.ds(slots * blocks + p, chips, stride=rows), :] = pair
    for r in range(slots * blocks + slots // 2, rows):
        scr[pl.ds(r, chips, stride=rows), :] = tags
    out_ref[...] = scr[...].astype(bf16).reshape(chips, tiles, 4, LANES)

    aux_ref[...] = jnp.zeros(aux_ref.shape, f32)
    aux_ref[:held, :pairs] = ms_ref[...]
    aux_ref[held : 2 * held, :pairs] = vs_ref[...]
    count = count_ref[...] + 1
    for at, beta in ((2 * held, beta_one), (2 * held + 1, beta_two)):
        power = jnp.ones(count.shape, f32)
        for bit in range(8):
            power = jnp.where((count >> bit) % 2 == 1, power * beta ** (1 << bit), power)
        aux_ref[at : at + 1, :held] = 1.0 / (1.0 - power)
    state_row = iota((state_rows, held), 0) - held * owner
    mine = jnp.where(state_row == iota((state_rows, held), 1), trained, 0.0)
    aux_ref[2 * held + 2 : 2 * held + 3, :held] = jnp.max(mine, axis=0, keepdims=True)


def pack(slots, offset, core, owner, ids, slot_of, active, counts, m_scale, v_scale, features, cotangent, chips):
    blocks = features.shape[1] // LANES
    rows = message_rows(slots, blocks)
    return pl.pallas_call(
        functools.partial(pack_kernel, slots, offset),
        out_shape=(
            jax.ShapeDtypeStruct((chips, rows // 4, 4, LANES), features.dtype),
            jax.ShapeDtypeStruct((8, LANES), jnp.float32),
        ),
        in_specs=[SMEM, SMEM] + [VMEM] * 6 + [ANY, VMEM],
        out_specs=(VMEM, VMEM),
        scratch_shapes=[
            pltpu.VMEM((chips * rows, LANES), jnp.float32),
            pltpu.VMEM(features.shape, features.dtype),
            pltpu.SemaphoreType.DMA,
        ],
        compiler_params=GRANT,
        name=f"pack{slots}",
    )(core, owner, ids, slot_of, active, counts, m_scale, v_scale, features, cotangent)


def grad_kernel(slots, in_ref, own_ref, other_ref, flag_ref, scr):
    chips, tiles = in_ref.shape[0], in_ref.shape[1]
    rows = tiles * 4
    half, columns = own_ref.shape
    rank = half // 2
    blocks = columns // LANES
    f32, bf16 = jnp.float32, jnp.bfloat16
    scr[...] = in_ref[...].reshape(chips * rows, LANES).astype(f32)
    low = iota((chips, LANES), 1) < rank
    tags = scr[pl.ds(rows - 1, chips, stride=rows), :]
    weights, wide = [], []
    for i in range(slots):
        pair = scr[pl.ds(slots * blocks + i // 2, chips, stride=rows), :]
        one = jnp.where(low if i % 2 == 0 else ~low, pair, 0.0)
        both = one + pltpu.roll(one, rank, 1)
        h = [tags[:, 4 * i + l : 4 * i + l + 1] for l in range(4)]
        weights.append(
            jnp.concatenate(
                [both * jnp.where(low, h[0], h[1]), both * jnp.where(low, h[2], h[3])], axis=1
            ).astype(bf16)
        )
        wide.append(
            jnp.concatenate(
                [scr[pl.ds(i * blocks + b, chips, stride=rows), :] for b in range(blocks)], axis=1
            ).astype(bf16)
        )
    total = lax.dot_general(
        jnp.concatenate(weights, axis=0),
        jnp.concatenate(wide, axis=0),
        (((0,), (0,)), ((), ())),
        preferred_element_type=f32,
    )
    own_ref[...] = total[:half]
    other_ref[:half, :] = total[half:]
    more = jnp.max(tags[:, 4 * slots : 4 * slots + 1], axis=0, keepdims=True)
    other_ref[half:, :] = jnp.broadcast_to(more, (8, columns))
    flag_ref[...] = jnp.broadcast_to(more, flag_ref.shape)


def partial_gradients(slots, received, half, columns):
    chips, tiles = received.shape[0], received.shape[1]
    f32 = jnp.float32
    return pl.pallas_call(
        functools.partial(grad_kernel, slots),
        out_shape=(
            jax.ShapeDtypeStruct((half, columns), f32),
            jax.ShapeDtypeStruct((half + 8, columns), f32),
            jax.ShapeDtypeStruct((8, LANES), f32),
        ),
        in_specs=[VMEM],
        out_specs=(VMEM, VMEM, VMEM),
        scratch_shapes=[pltpu.VMEM((chips * tiles * 4, LANES), f32)],
        compiler_params=GRANT,
        name=f"grad{slots}",
    )(received)


def moments(j, aux_ref, gradient, mc_ref, vc_ref, spread):
    f32 = jnp.float32
    held, rank, _ = mc_ref.shape
    pairs = rank // 2

    def per_row(at):
        return jnp.sum(jnp.where(spread, aux_ref[at : at + 1, :pairs], 0.0), axis=1, keepdims=True)

    moment = mc_ref[j].astype(f32) * (beta_one * per_row(j)) + (1.0 - beta_one) * gradient
    second = vc_ref[j].astype(f32) * (beta_two * per_row(held + j)) + (1.0 - beta_two) * gradient * gradient
    inverse_one = aux_ref[2 * held : 2 * held + 1, j : j + 1]
    inverse_two = aux_ref[2 * held + 1 : 2 * held + 2, j : j + 1]
    direction = (moment * inverse_one) / (jnp.sqrt(second * inverse_two) + adam_eps)
    return moment, second, direction


def row_spread(rank):
    return iota((rank, rank // 2), 0) // 2 == iota((rank, rank // 2), 1)


def trained_row(aux_ref, held, j, shape):
    return jnp.broadcast_to(aux_ref[2 * held + 2 : 2 * held + 3, j : j + 1], shape) > 0


def serve_kernel(
    aux_ref, own_ref, other_ref, flag_ref, weight_ref, mc_ref, vc_ref,
    served_hbm, total_ref, more_ref, out_ref, sems,
):
    held, rank, columns = weight_ref.shape
    spread = row_spread(rank)
    more_ref[...] = flag_ref[...] + other_ref[held * rank :, :LANES]
    sends = []
    for j in range(held):
        at = slice(j * rank, (j + 1) * rank)
        gradient = own_ref[at, :] + other_ref[at, :]
        total_ref[at, :] = gradient
        _, _, direction = moments(j, aux_ref, gradient, mc_ref, vc_ref, spread)
        weight = weight_ref[j].astype(jnp.float32)
        served = weight - learn_rate * (direction + decay_rate * weight)
        served = jnp.where(trained_row(aux_ref, held, j, weight.shape), served, weight)
        out_ref[j] = served.astype(out_ref.dtype)
        for r in range(served_hbm.shape[0]):
            send = pltpu.make_async_copy(out_ref.at[j], served_hbm.at[r, j], sems.at[j, r])
            send.start()
            sends.append(send)
    for send in sends:
        send.wait()


def serve(replicas, aux, own, other, flag, weight, m_code, v_code):
    held = weight.shape[0]
    like = jax.ShapeDtypeStruct
    return pl.pallas_call(
        serve_kernel,
        out_shape=(
            like((replicas, *weight.shape), weight.dtype),
            like(own.shape, jnp.float32),
            like(flag.shape, jnp.float32),
        ),
        in_specs=[VMEM] * 7,
        out_specs=(ANY, VMEM, VMEM),
        scratch_shapes=[
            pltpu.VMEM(weight.shape, weight.dtype),
            pltpu.SemaphoreType.DMA((held, replicas)),
        ],
        compiler_params=GRANT,
        name="serve",
    )(aux, own, other, flag, weight, m_code, v_code)


def state_kernel(
    aux_ref, total_ref, flag_ref, mc_ref, vc_ref, dir_ref, mc_out, ms_out, vc_out, vs_out, more_ref
):
    f32 = jnp.float32
    held, rank, columns = mc_ref.shape
    pairs = rank // 2
    spread = row_spread(rank)

    def per_pair(values):
        return jnp.max(jnp.where(spread, values, 0.0), axis=0, keepdims=True)

    def per_row(scales):
        return jnp.sum(jnp.where(spread, scales, 0.0), axis=1, keepdims=True)

    more_ref[...] = flag_ref[...]
    for j in range(held):
        gradient = total_ref[j * rank : (j + 1) * rank, :]
        moment, second, direction = moments(j, aux_ref, gradient, mc_ref, vc_ref, spread)
        keep = trained_row(aux_ref, held, j, moment.shape)
        keep_row = trained_row(aux_ref, held, j, (1, pairs))
        m_new = per_pair(jnp.max(jnp.abs(moment), axis=1, keepdims=True)) + scale_eps
        v_new = per_pair(jnp.max(second, axis=1, keepdims=True)) + scale_eps
        dir_ref[j] = jnp.where(keep, direction, 0.0)
        m_code, v_code = moment / per_row(m_new), second / per_row(v_new)
        mc_out[j] = jnp.where(keep, m_code, mc_ref[j].astype(f32)).astype(mc_out.dtype)
        vc_out[j] = jnp.where(keep, v_code, vc_ref[j].astype(f32)).astype(vc_out.dtype)
        ms_out[j : j + 1, :] = jnp.where(keep_row, m_new, aux_ref[j : j + 1, :pairs])
        vs_out[j : j + 1, :] = jnp.where(keep_row, v_new, aux_ref[held + j : held + j + 1, :pairs])


def state(aux, total, flag, m_code, v_code):
    f32 = jnp.float32
    like = jax.ShapeDtypeStruct
    scales = like((m_code.shape[0], m_code.shape[1] // 2), f32)
    return pl.pallas_call(
        state_kernel,
        out_shape=(
            like(m_code.shape, f32),
            like(m_code.shape, m_code.dtype),
            scales,
            like(v_code.shape, v_code.dtype),
            scales,
            like(flag.shape, f32),
        ),
        in_specs=[VMEM] * 5,
        out_specs=(VMEM,) * 6,
        compiler_params=GRANT,
        name="state",
    )(aux, total, flag, m_code, v_code)


def on_device(
    features, cotangent, adapter_ids, slot_of, active_ids, step_counts,
    weight, m_code, m_scale, v_code, v_scale,
):
    columns = features.shape[1]
    held, rank = weight.shape[0], weight.shape[1]
    half = held * rank
    chips = lax.axis_size(("x", "z"))
    replicas = lax.axis_size("replica")
    core = lax.axis_index("core").astype(jnp.int32).reshape(1)
    owner = lax.axis_index(("x", "z", "core")).astype(jnp.int32).reshape(1)
    arrays = (
        adapter_ids.reshape(1, -1), slot_of.reshape(1, -1), active_ids.reshape(1, -1), step_counts.reshape(1, -1),
        m_scale.reshape(held, -1), v_scale.reshape(held, -1), features, cotangent.T,
    )
    swap = [(0, 1), (1, 0)]

    def exchange(slots, offset, core):
        sent, aux = pack(slots, offset, core, owner, *arrays, chips)
        received = lax.all_to_all(sent, ("x", "z"), split_axis=0, concat_axis=0, tiled=True)
        own, other, flag = partial_gradients(slots, received, half, columns)
        return own, lax.ppermute(other, "core", swap), flag, aux

    def update(own, other, flag, aux):
        copies, total, more = serve(replicas, aux, own, other, flag, weight, m_code, v_code)
        parts = lax.all_to_all(copies, "replica", split_axis=0, concat_axis=0, tiled=True)
        served = jnp.moveaxis(parts, 0, 2).reshape(held, rank, -1)
        direction, m_new, ms_new, v_new, vs_new, more = state(aux, total, more, m_code, v_code)
        return total, (more[0, 0], direction, m_new, ms_new, v_new, vs_new, served)

    total, results = update(*exchange(FIRST, 0, core))

    def with_the_rest(carry):
        here = core + (carry[0] < 0).astype(jnp.int32)
        own, other, flag, aux = exchange(8 - FIRST, FIRST, here)
        return update(total + own, other, flag, aux)[1]

    results = lax.while_loop(lambda carry: carry[0] > 0, with_the_rest, results)
    _, direction, m_new, ms_new, v_new, vs_new, served = results
    return (
        direction, m_new, ms_new.reshape(m_scale.shape), v_new, vs_new.reshape(v_scale.shape), served,
    )


def solution(mesh):
    owners, replicas = mesh.devices.shape
    fine = Mesh(mesh.devices.reshape(4, owners // 8, 2, replicas), ("x", "z", "core", "replica"))
    owner = ("x", "z", "core")
    block = P(owner, None, "replica")
    return jax.shard_map(
        on_device,
        mesh=fine,
        in_specs=(
            P(owner, "replica"), P(owner, None), P(owner, None), P(), P(), P(owner),
            block, block, block, block, block,
        ),
        out_specs=(block, block, block, block, block, P(owner, None, None)),
        check_vma=False,
    )
```

```python
import functools

import jax
import jax.numpy as jnp
from jax import lax
from jax.experimental import pallas as pl
from jax.experimental.pallas import tpu as pltpu
from jax.sharding import Mesh
from jax.sharding import PartitionSpec as P

beta_one = 0.9
beta_two = 0.999
adam_eps = 1e-08
scale_eps = 1e-06
learn_rate = 0.001
decay_rate = 0.01

LANES = 128
FIRST = 6
VMEM = pl.BlockSpec(memory_space=pltpu.VMEM)
SMEM = pl.BlockSpec(memory_space=pltpu.SMEM)
ANY = pl.BlockSpec(memory_space=pl.ANY)
GRANT = pltpu.CompilerParams(vmem_limit_bytes=16 << 20)


def message_rows(slots, blocks):
    rows = slots * blocks + (slots + 1) // 2 + 1
    return -(-rows // 4) * 4


def iota(shape, dim):
    return lax.broadcasted_iota(jnp.int32, shape, dim)


def pack_kernel(
    slots, core_ref, owner_ref, offset_ref, ids_ref, slot_ref, act_ref, count_ref, ms_ref, vs_ref, cot_ref, feat_hbm,
    out_ref, aux_ref, scr, feat_ref, feat_sem,
):
    fetch = pltpu.make_async_copy(feat_hbm, feat_ref, feat_sem)
    fetch.start()
    rank, tokens = cot_ref.shape
    state_rows = slot_ref.shape[1]
    columns = feat_ref.shape[1]
    chips, tiles = out_ref.shape[0], out_ref.shape[1]
    rows, blocks = tiles * 4, columns // LANES
    held, pairs = ms_ref.shape
    f32, bf16 = jnp.float32, jnp.bfloat16
    dot = functools.partial(jnp.dot, preferred_element_type=f32)
    here, owner, offset = core_ref[0], owner_ref[0], offset_ref[0].astype(f32)

    square = (state_rows, state_rows)
    named = slot_ref[...] == iota(square, 0)
    adapter = jnp.sum(jnp.where(named, iota(square, 1), 0).astype(f32), axis=1, keepdims=True)
    adapter = adapter.astype(jnp.int32)
    trained = jnp.max((act_ref[...] == adapter).astype(f32), axis=1, keepdims=True)
    place = jnp.where(ids_ref[...] == adapter, trained, 0.0).astype(bf16)
    of_chip = (iota((chips, state_rows), 1) // 4 == iota((chips, state_rows), 0)).astype(f32).astype(bf16)
    member = dot(of_chip, place)
    earlier = (iota((tokens, tokens), 0) < iota((tokens, tokens), 1)).astype(f32).astype(bf16)
    before = dot(member.astype(bf16), earlier) - offset
    late = jnp.where((member > 0) & (before >= slots), 1.0, 0.0)
    more = jnp.max(jnp.max(late, axis=1, keepdims=True), axis=0, keepdims=True)
    chosen = jnp.concatenate([jnp.where(before == i, member, 0.0).astype(bf16) for i in range(slots)], axis=0)

    local = (iota((state_rows, LANES), 0) + 2 * here) % 4
    tag = (iota((state_rows, LANES), 1) == rank + local).astype(f32).astype(bf16)
    embed = (iota((rank, LANES), 0) == iota((rank, LANES), 1)).astype(f32).astype(bf16)
    beside = lax.dot_general(
        jnp.concatenate([cot_ref[...], place], axis=0),
        jnp.concatenate([embed, tag], axis=0),
        (((0,), (0,)), ((), ())),
        preferred_element_type=f32,
    )
    beside = dot(chosen, beside.astype(bf16))
    fetch.wait()
    moved = dot(chosen, feat_ref[...])
    of_slot = [slice(i * chips, (i + 1) * chips) for i in range(slots)]
    for i in range(slots):
        for b in range(blocks):
            scr[pl.ds(i * blocks + b, chips, stride=rows), :] = moved[of_slot[i], b * LANES : (b + 1) * LANES]
    lane = iota((chips, LANES), 1)
    tags = jnp.where(lane == 4 * slots, more, 0.0)
    for i in range(slots):
        one = jnp.where((lane >= rank) & (lane < rank + 4), beside[of_slot[i]], 0.0)
        tags = tags + pltpu.roll(one, (LANES - rank + 4 * i) % LANES, 1)
    for p in range((slots + 1) // 2):
        pair = jnp.where(lane < rank, beside[of_slot[2 * p]], 0.0)
        if 2 * p + 1 < slots:
            pair = jnp.where(lane < rank, pair, pltpu.roll(beside[of_slot[2 * p + 1]], rank, 1))
        scr[pl.ds(slots * blocks + p, chips, stride=rows), :] = pair
    for r in range(slots * blocks + (slots + 1) // 2, rows):
        scr[pl.ds(r, chips, stride=rows), :] = tags
    out_ref[...] = scr[...].astype(out_ref.dtype).reshape(chips, tiles, 4, LANES)

    aux_ref[...] = jnp.zeros(aux_ref.shape, f32)
    aux_ref[:held, :pairs] = ms_ref[...]
    aux_ref[held : 2 * held, :pairs] = vs_ref[...]
    count = count_ref[...] + 1
    for at, beta in ((2 * held, beta_one), (2 * held + 1, beta_two)):
        power = jnp.ones(count.shape, f32)
        for bit in range(8):
            power = jnp.where((count >> bit) % 2 == 1, power * beta ** (1 << bit), power)
        aux_ref[at : at + 1, :held] = 1.0 / (1.0 - power)
    state_row = iota((state_rows, held), 0) - held * owner
    mine = jnp.where(state_row == iota((state_rows, held), 1), trained, 0.0)
    aux_ref[2 * held + 2 : 2 * held + 3, :held] = jnp.max(mine, axis=0, keepdims=True)


def pack(slots, chips, core, owner, offset, small, cotangent, features):
    rows = message_rows(slots, features.shape[1] // LANES)
    like = jax.ShapeDtypeStruct
    return pl.pallas_call(
        functools.partial(pack_kernel, slots),
        out_shape=(like((chips, rows // 4, 4, LANES), features.dtype), like((8, LANES), jnp.float32)),
        in_specs=[SMEM] * 3 + [VMEM] * 7 + [ANY],
        out_specs=(VMEM, VMEM),
        scratch_shapes=[
            pltpu.VMEM((chips * rows, LANES), jnp.float32),
            pltpu.VMEM(features.shape, features.dtype),
            pltpu.SemaphoreType.DMA,
        ],
        compiler_params=GRANT,
        name=f"pack{slots}",
    )(core, owner, offset, *small, cotangent, features)


def grad_kernel(slots, offset_ref, in_ref, own_ref, other_ref, next_ref, scr):
    chips, tiles = in_ref.shape[0], in_ref.shape[1]
    rows = tiles * 4
    half, columns = own_ref.shape
    rank = half // 2
    blocks = columns // LANES
    f32, bf16 = jnp.float32, jnp.bfloat16
    scr[...] = in_ref[...].reshape(chips * rows, LANES).astype(f32)
    low = iota((chips, LANES), 1) < rank
    tags = scr[pl.ds(rows - 1, chips, stride=rows), :]
    more = jnp.max(tags[:, 4 * slots : 4 * slots + 1]) > 0
    next_ref[0] = jnp.where(more, offset_ref[0] + slots, 0)
    weights, wide = [], []
    for i in range(slots):
        pair = scr[pl.ds(slots * blocks + i // 2, chips, stride=rows), :]
        one = jnp.where(low if i % 2 == 0 else ~low, pair, 0.0)
        both = one + pltpu.roll(one, rank, 1)
        h = [tags[:, 4 * i + l : 4 * i + l + 1] for l in range(4)]
        weights.append(
            jnp.concatenate(
                [both * jnp.where(low, h[0], h[1]), both * jnp.where(low, h[2], h[3])], axis=1
            ).astype(bf16)
        )
        wide.append(
            jnp.concatenate(
                [scr[pl.ds(i * blocks + b, chips, stride=rows), :] for b in range(blocks)], axis=1
            ).astype(bf16)
        )
    total = lax.dot_general(
        jnp.concatenate(weights, axis=0),
        jnp.concatenate(wide, axis=0),
        (((0,), (0,)), ((), ())),
        preferred_element_type=f32,
    )
    own_ref[...] = total[:half]
    other_ref[...] = total[half:]


def partial_gradients(slots, offset, received, half, columns):
    chips, tiles = received.shape[0], received.shape[1]
    f32 = jnp.float32
    return pl.pallas_call(
        functools.partial(grad_kernel, slots),
        out_shape=(
            jax.ShapeDtypeStruct((half, columns), f32),
            jax.ShapeDtypeStruct((half, columns), f32),
            jax.ShapeDtypeStruct((1,), jnp.int32),
        ),
        in_specs=[SMEM, VMEM],
        out_specs=(VMEM, VMEM, SMEM),
        scratch_shapes=[pltpu.VMEM((chips * tiles * 4, LANES), f32)],
        compiler_params=GRANT,
        name=f"grad{slots}",
    )(offset, received)


def moments(j, aux_ref, gradient, mc_ref, vc_ref, spread):
    f32 = jnp.float32
    held, rank, _ = mc_ref.shape
    pairs = rank // 2

    def per_row(at):
        return jnp.sum(jnp.where(spread, aux_ref[at : at + 1, :pairs], 0.0), axis=1, keepdims=True)

    moment = mc_ref[j].astype(f32) * (beta_one * per_row(j)) + (1.0 - beta_one) * gradient
    second = vc_ref[j].astype(f32) * (beta_two * per_row(held + j)) + (1.0 - beta_two) * gradient * gradient
    inverse_one = aux_ref[2 * held : 2 * held + 1, j : j + 1]
    inverse_two = aux_ref[2 * held + 1 : 2 * held + 2, j : j + 1]
    direction = (moment * inverse_one) / (jnp.sqrt(second * inverse_two) + adam_eps)
    return moment, second, direction


def row_spread(rank):
    return iota((rank, rank // 2), 0) // 2 == iota((rank, rank // 2), 1)


def trained_row(aux_ref, held, j, shape):
    return jnp.broadcast_to(aux_ref[2 * held + 2 : 2 * held + 3, j : j + 1], shape) > 0


def serve_kernel(aux_ref, own_ref, other_ref, weight_ref, mc_ref, vc_ref, served_hbm, total_ref, out_ref, sems):
    held, rank, columns = weight_ref.shape
    spread = row_spread(rank)
    sends = []
    for j in range(held):
        at = slice(j * rank, (j + 1) * rank)
        gradient = own_ref[at, :] + other_ref[at, :]
        total_ref[at, :] = gradient
        _, _, direction = moments(j, aux_ref, gradient, mc_ref, vc_ref, spread)
        weight = weight_ref[j].astype(jnp.float32)
        served = weight - learn_rate * (direction + decay_rate * weight)
        served = jnp.where(trained_row(aux_ref, held, j, weight.shape), served, weight)
        out_ref[j] = served.astype(out_ref.dtype)
        for r in range(served_hbm.shape[0]):
            send = pltpu.make_async_copy(out_ref.at[j], served_hbm.at[r, j], sems.at[j, r])
            send.start()
            sends.append(send)
    for send in sends:
        send.wait()


def serve(replicas, aux, own, other, weight, m_code, v_code):
    held = weight.shape[0]
    like = jax.ShapeDtypeStruct
    return pl.pallas_call(
        serve_kernel,
        out_shape=(like((replicas, *weight.shape), weight.dtype), like(own.shape, jnp.float32)),
        in_specs=[VMEM] * 6,
        out_specs=(ANY, VMEM),
        scratch_shapes=[
            pltpu.VMEM(weight.shape, weight.dtype),
            pltpu.SemaphoreType.DMA((held, replicas)),
        ],
        compiler_params=GRANT,
        name="serve",
    )(aux, own, other, weight, m_code, v_code)


def assemble_kernel(parts_ref, out_ref, sems):
    replicas, columns = parts_ref.shape[0], parts_ref.shape[3]
    moves = [
        pltpu.make_async_copy(parts_ref.at[r], out_ref.at[:, :, pl.ds(r * columns, columns)], sems.at[r])
        for r in range(replicas)
    ]
    for move in moves:
        move.start()
    for move in moves:
        move.wait()


def assemble(parts):
    replicas, held, rank, columns = parts.shape
    return pl.pallas_call(
        assemble_kernel,
        out_shape=jax.ShapeDtypeStruct((held, rank, replicas * columns), parts.dtype),
        in_specs=[ANY],
        out_specs=ANY,
        scratch_shapes=[pltpu.SemaphoreType.DMA((replicas,))],
        compiler_params=GRANT,
        name="assemble",
    )(parts)


def state_kernel(
    aux_ref, total_ref, mc_ref, vc_ref, dir_ref, mc_out, ms_out, vc_out, vs_out
):
    f32 = jnp.float32
    held, rank, columns = mc_ref.shape
    pairs = rank // 2
    spread = row_spread(rank)

    def per_pair(values):
        return jnp.max(jnp.where(spread, values, 0.0), axis=0, keepdims=True)

    def per_row(scales):
        return jnp.sum(jnp.where(spread, scales, 0.0), axis=1, keepdims=True)

    for j in range(held):
        gradient = total_ref[j * rank : (j + 1) * rank, :]
        moment, second, direction = moments(j, aux_ref, gradient, mc_ref, vc_ref, spread)
        keep = trained_row(aux_ref, held, j, moment.shape)
        keep_row = trained_row(aux_ref, held, j, (1, pairs))
        m_new = per_pair(jnp.max(jnp.abs(moment), axis=1, keepdims=True)) + scale_eps
        v_new = per_pair(jnp.max(second, axis=1, keepdims=True)) + scale_eps
        dir_ref[j] = jnp.where(keep, direction, 0.0)
        m_code, v_code = moment / per_row(m_new), second / per_row(v_new)
        mc_out[j] = jnp.where(keep, m_code, mc_ref[j].astype(f32)).astype(mc_out.dtype)
        vc_out[j] = jnp.where(keep, v_code, vc_ref[j].astype(f32)).astype(vc_out.dtype)
        ms_out[j : j + 1, :] = jnp.where(keep_row, m_new, aux_ref[j : j + 1, :pairs])
        vs_out[j : j + 1, :] = jnp.where(keep_row, v_new, aux_ref[held + j : held + j + 1, :pairs])


def state(aux, total, m_code, v_code):
    f32 = jnp.float32
    like = jax.ShapeDtypeStruct
    scales = like((m_code.shape[0], m_code.shape[1] // 2), f32)
    return pl.pallas_call(
        state_kernel,
        out_shape=(
            like(m_code.shape, f32),
            like(m_code.shape, m_code.dtype),
            scales,
            like(v_code.shape, v_code.dtype),
            scales,
        ),
        in_specs=[VMEM] * 4,
        out_specs=(VMEM,) * 5,
        compiler_params=GRANT,
        name="state",
    )(aux, total, m_code, v_code)


def on_device(
    features, cotangent, adapter_ids, slot_of, active_ids, step_counts,
    weight, m_code, m_scale, v_code, v_scale,
):
    columns = features.shape[1]
    held, rank = weight.shape[0], weight.shape[1]
    half = held * rank
    chips = lax.axis_size(("x", "z"))
    replicas = lax.axis_size("replica")
    core = lax.axis_index("core").astype(jnp.int32).reshape(1)
    owner = lax.axis_index(("x", "z", "core")).astype(jnp.int32).reshape(1)
    small = (
        adapter_ids.reshape(1, -1), slot_of.reshape(1, -1), active_ids.reshape(1, -1), step_counts.reshape(1, -1),
        m_scale.reshape(held, -1), v_scale.reshape(held, -1),
    )

    def exchange(slots, offset):
        sent, aux = pack(slots, chips, core, owner, offset, small, cotangent.T, features)
        received = lax.all_to_all(sent, ("x", "z"), split_axis=0, concat_axis=0, tiled=True)
        return partial_gradients(slots, offset, received, half, columns), aux

    def another(carry):
        own, other, rank_next = carry
        (more_own, more_other, rank_next), _ = exchange(1, rank_next)
        return own + more_own, other + more_other, rank_next

    carry, aux = exchange(FIRST, jnp.zeros((1,), jnp.int32))
    own, other, _ = lax.while_loop(lambda carry: carry[2][0] > 0, another, carry)
    other = lax.ppermute(other, "core", [(0, 1), (1, 0)])
    copies, total = serve(replicas, aux, own, other, weight, m_code, v_code)
    parts = lax.all_to_all(copies, "replica", split_axis=0, concat_axis=0, tiled=True)
    direction, m_new, ms_new, v_new, vs_new = state(aux, total, m_code, v_code)
    served = assemble(parts)
    return (
        direction, m_new, ms_new.reshape(m_scale.shape), v_new, vs_new.reshape(v_scale.shape), served,
    )


def solution(mesh):
    owners, replicas = mesh.devices.shape
    fine = Mesh(mesh.devices.reshape(4, owners // 8, 2, replicas), ("x", "z", "core", "replica"))
    owner = ("x", "z", "core")
    block = P(owner, None, "replica")
    return jax.shard_map(
        on_device,
        mesh=fine,
        in_specs=(
            P(owner, "replica"), P(owner, None), P(owner, None), P(), P(), P(owner),
            block, block, block, block, block,
        ),
        out_specs=(block, block, block, block, block, P(owner, None, None)),
        check_vma=False,
    )
```

```python
import functools

import jax
import jax.numpy as jnp
from jax import lax
from jax.experimental import pallas as pl
from jax.experimental.pallas import tpu as pltpu
from jax.sharding import Mesh
from jax.sharding import PartitionSpec as P

beta_one = 0.9
beta_two = 0.999
adam_eps = 1e-08
scale_eps = 1e-06
learn_rate = 0.001
decay_rate = 0.01

LANES = 128
PIECES = 2
FIRST = 6
VMEM = pl.BlockSpec(memory_space=pltpu.VMEM)
SMEM = pl.BlockSpec(memory_space=pltpu.SMEM)
ANY = pl.BlockSpec(memory_space=pl.ANY)
GRANT = pltpu.CompilerParams(vmem_limit_bytes=16 << 20)


def message_rows(slots, blocks):
    rows = slots * blocks + (slots + 1) // 2 + 1
    return -(-rows // 4) * 4


def iota(shape, dim):
    return lax.broadcasted_iota(jnp.int32, shape, dim)


def pack_kernel(
    slots, core_ref, owner_ref, offset_ref, ids_ref, slot_ref, act_ref, count_ref, ms_ref, vs_ref, cot_ref, feat_hbm,
    out_ref, aux_ref, scr, feat_ref, feat_sem,
):
    fetch = pltpu.make_async_copy(feat_hbm, feat_ref, feat_sem)
    fetch.start()
    rank, tokens = cot_ref.shape
    state_rows = slot_ref.shape[1]
    columns = feat_ref.shape[1]
    chips, tiles = out_ref.shape[0], out_ref.shape[1]
    rows, blocks = tiles * 4, columns // LANES
    held, pairs = ms_ref.shape
    f32, bf16 = jnp.float32, jnp.bfloat16
    dot = functools.partial(jnp.dot, preferred_element_type=f32)
    here, owner, offset = core_ref[0], owner_ref[0], offset_ref[0].astype(f32)

    square = (state_rows, state_rows)
    named = slot_ref[...] == iota(square, 0)
    adapter = jnp.sum(jnp.where(named, iota(square, 1), 0).astype(f32), axis=1, keepdims=True)
    adapter = adapter.astype(jnp.int32)
    trained = jnp.max((act_ref[...] == adapter).astype(f32), axis=1, keepdims=True)
    place = jnp.where(ids_ref[...] == adapter, trained, 0.0).astype(bf16)
    of_chip = (iota((chips, state_rows), 1) // 4 == iota((chips, state_rows), 0)).astype(f32).astype(bf16)
    member = dot(of_chip, place)
    earlier = (iota((tokens, tokens), 0) < iota((tokens, tokens), 1)).astype(f32).astype(bf16)
    before = dot(member.astype(bf16), earlier) - offset
    late = jnp.where((member > 0) & (before >= slots), 1.0, 0.0)
    more = jnp.max(jnp.max(late, axis=1, keepdims=True), axis=0, keepdims=True)
    chosen = jnp.concatenate([jnp.where(before == i, member, 0.0).astype(bf16) for i in range(slots)], axis=0)

    local = (iota((state_rows, LANES), 0) + 2 * here) % 4
    tag = (iota((state_rows, LANES), 1) == rank + local).astype(f32).astype(bf16)
    embed = (iota((rank, LANES), 0) == iota((rank, LANES), 1)).astype(f32).astype(bf16)
    beside = lax.dot_general(
        jnp.concatenate([cot_ref[...], place], axis=0),
        jnp.concatenate([embed, tag], axis=0),
        (((0,), (0,)), ((), ())),
        preferred_element_type=f32,
    )
    beside = dot(chosen, beside.astype(bf16))
    of_slot = [slice(i * chips, (i + 1) * chips) for i in range(slots)]
    lane = iota((chips, LANES), 1)
    tags = jnp.where(lane == 4 * slots, more, 0.0)
    for i in range(slots):
        one = jnp.where((lane >= rank) & (lane < rank + 4), beside[of_slot[i]], 0.0)
        tags = tags + pltpu.roll(one, (LANES - rank + 4 * i) % LANES, 1)
    for p in range((slots + 1) // 2):
        pair = jnp.where(lane < rank, beside[of_slot[2 * p]], 0.0)
        if 2 * p + 1 < slots:
            pair = jnp.where(lane < rank, pair, pltpu.roll(beside[of_slot[2 * p + 1]], rank, 1))
        scr[pl.ds(slots * blocks + p, chips, stride=rows), :] = pair
    for r in range(slots * blocks + (slots + 1) // 2, rows):
        scr[pl.ds(r, chips, stride=rows), :] = tags

    aux_ref[...] = jnp.zeros(aux_ref.shape, f32)
    aux_ref[:held, :pairs] = ms_ref[...]
    aux_ref[held : 2 * held, :pairs] = vs_ref[...]
    count = count_ref[...] + 1
    for at, beta in ((2 * held, beta_one), (2 * held + 1, beta_two)):
        power = jnp.ones(count.shape, f32)
        for bit in range(8):
            power = jnp.where((count >> bit) % 2 == 1, power * beta ** (1 << bit), power)
        aux_ref[at : at + 1, :held] = 1.0 / (1.0 - power)
    state_row = iota((state_rows, held), 0) - held * owner
    mine = jnp.where(state_row == iota((state_rows, held), 1), trained, 0.0)
    aux_ref[2 * held + 2 : 2 * held + 3, :held] = jnp.max(mine, axis=0, keepdims=True)

    fetch.wait()
    moved = dot(chosen, feat_ref[...])
    for i in range(slots):
        for b in range(blocks):
            scr[pl.ds(i * blocks + b, chips, stride=rows), :] = moved[of_slot[i], b * LANES : (b + 1) * LANES]
    out_ref[...] = scr[...].astype(out_ref.dtype).reshape(chips, tiles, 4, LANES)


def pack(slots, chips, core, owner, offset, small, cotangent, features):
    rows = message_rows(slots, features.shape[1] // LANES)
    like = jax.ShapeDtypeStruct
    return pl.pallas_call(
        functools.partial(pack_kernel, slots),
        out_shape=(like((chips, rows // 4, 4, LANES), features.dtype), like((8, LANES), jnp.float32)),
        in_specs=[SMEM] * 3 + [VMEM] * 7 + [ANY],
        out_specs=(VMEM, VMEM),
        scratch_shapes=[
            pltpu.VMEM((chips * rows, LANES), jnp.float32),
            pltpu.VMEM(features.shape, features.dtype),
            pltpu.SemaphoreType.DMA,
        ],
        compiler_params=GRANT,
        name=f"pack{slots}",
    )(core, owner, offset, *small, cotangent, features)


def grad_kernel(slots, offset_ref, in_ref, own_ref, other_ref, next_ref, scr):
    chips, tiles = in_ref.shape[0], in_ref.shape[1]
    rows = tiles * 4
    half, columns = own_ref.shape
    rank = half // 2
    blocks = columns // LANES
    f32, bf16 = jnp.float32, jnp.bfloat16
    scr[...] = in_ref[...].reshape(chips * rows, LANES).astype(f32)
    low = iota((chips, LANES), 1) < rank
    tags = scr[pl.ds(rows - 1, chips, stride=rows), :]
    more = jnp.max(tags[:, 4 * slots : 4 * slots + 1]) > 0
    next_ref[0] = jnp.where(more, offset_ref[0] + slots, 0)
    weights, wide = [], []
    for i in range(slots):
        pair = scr[pl.ds(slots * blocks + i // 2, chips, stride=rows), :]
        one = jnp.where(low if i % 2 == 0 else ~low, pair, 0.0)
        both = one + pltpu.roll(one, rank, 1)
        h = [tags[:, 4 * i + l : 4 * i + l + 1] for l in range(4)]
        weights.append(
            jnp.concatenate(
                [both * jnp.where(low, h[0], h[1]), both * jnp.where(low, h[2], h[3])], axis=1
            ).astype(bf16)
        )
        wide.append(
            jnp.concatenate(
                [scr[pl.ds(i * blocks + b, chips, stride=rows), :] for b in range(blocks)], axis=1
            ).astype(bf16)
        )
    total = lax.dot_general(
        jnp.concatenate(weights, axis=0),
        jnp.concatenate(wide, axis=0),
        (((0,), (0,)), ((), ())),
        preferred_element_type=f32,
    )
    own_ref[...] = total[:half]
    other_ref[...] = total[half:]


def partial_gradients(slots, offset, received, half, columns):
    chips, tiles = received.shape[0], received.shape[1]
    f32 = jnp.float32
    return pl.pallas_call(
        functools.partial(grad_kernel, slots),
        out_shape=(
            jax.ShapeDtypeStruct((half, columns), f32),
            jax.ShapeDtypeStruct((half, columns), f32),
            jax.ShapeDtypeStruct((1,), jnp.int32),
        ),
        in_specs=[SMEM, VMEM],
        out_specs=(VMEM, VMEM, SMEM),
        scratch_shapes=[pltpu.VMEM((chips * tiles * 4, LANES), f32)],
        compiler_params=GRANT,
        name=f"grad{slots}",
    )(offset, received)


def moments(j, aux_ref, gradient, mc_ref, vc_ref, spread, at=slice(None)):
    f32 = jnp.float32
    held, rank, _ = mc_ref.shape
    pairs = rank // 2

    def per_row(at):
        return jnp.sum(jnp.where(spread, aux_ref[at : at + 1, :pairs], 0.0), axis=1, keepdims=True)

    moment = mc_ref[j, :, at].astype(f32) * (beta_one * per_row(j)) + (1.0 - beta_one) * gradient
    second = vc_ref[j, :, at].astype(f32) * (beta_two * per_row(held + j)) + (1.0 - beta_two) * gradient * gradient
    inverse_one = aux_ref[2 * held : 2 * held + 1, j : j + 1]
    inverse_two = aux_ref[2 * held + 1 : 2 * held + 2, j : j + 1]
    direction = (moment * inverse_one) / (jnp.sqrt(second * inverse_two) + adam_eps)
    return moment, second, direction


def row_spread(rank):
    return iota((rank, rank // 2), 0) // 2 == iota((rank, rank // 2), 1)


def trained_row(aux_ref, held, j, shape):
    return jnp.broadcast_to(aux_ref[2 * held + 2 : 2 * held + 3, j : j + 1], shape) > 0


def serve_kernel(aux_ref, own_ref, other_ref, weight_ref, mc_ref, vc_ref, served_hbm, total_ref, out_ref, sems):
    held, rank, columns = weight_ref.shape
    spread = row_spread(rank)
    width = columns // PIECES
    sends = []
    for n in range(held * PIECES):
        j, first = n // PIECES, n % PIECES * width
        rows, at = slice(j * rank, (j + 1) * rank), slice(first, first + width)
        gradient = own_ref[rows, at] + other_ref[rows, at]
        total_ref[rows, at] = gradient
        _, _, direction = moments(j, aux_ref, gradient, mc_ref, vc_ref, spread, at)
        weight = weight_ref[j, :, at].astype(jnp.float32)
        served = weight - learn_rate * (direction + decay_rate * weight)
        served = jnp.where(trained_row(aux_ref, held, j, weight.shape), served, weight)
        out_ref[j, :, at] = served.astype(out_ref.dtype)
        piece = (slice(None), pl.ds(first, width))
        for r in range(served_hbm.shape[0]):
            send = pltpu.make_async_copy(out_ref.at[j, *piece], served_hbm.at[r, j, *piece], sems.at[n, r])
            send.start()
            sends.append(send)
    for send in sends:
        send.wait()


def serve(replicas, aux, own, other, weight, m_code, v_code):
    held = weight.shape[0]
    like = jax.ShapeDtypeStruct
    return pl.pallas_call(
        serve_kernel,
        out_shape=(like((replicas, *weight.shape), weight.dtype), like(own.shape, jnp.float32)),
        in_specs=[VMEM] * 6,
        out_specs=(ANY, VMEM),
        scratch_shapes=[
            pltpu.VMEM(weight.shape, weight.dtype),
            pltpu.SemaphoreType.DMA((held * PIECES, replicas)),
        ],
        compiler_params=GRANT,
        name="serve",
    )(aux, own, other, weight, m_code, v_code)


def assemble_kernel(parts_ref, out_ref, sems):
    replicas, columns = parts_ref.shape[0], parts_ref.shape[3]
    moves = [
        pltpu.make_async_copy(parts_ref.at[r], out_ref.at[:, :, pl.ds(r * columns, columns)], sems.at[r])
        for r in range(replicas)
    ]
    for move in moves:
        move.start()
    for move in moves:
        move.wait()


def assemble(parts):
    replicas, held, rank, columns = parts.shape
    return pl.pallas_call(
        assemble_kernel,
        out_shape=jax.ShapeDtypeStruct((held, rank, replicas * columns), parts.dtype),
        in_specs=[ANY],
        out_specs=ANY,
        scratch_shapes=[pltpu.SemaphoreType.DMA((replicas,))],
        compiler_params=GRANT,
        name="assemble",
    )(parts)


def state_kernel(
    aux_ref, total_ref, mc_ref, vc_ref, dir_ref, mc_out, ms_out, vc_out, vs_out
):
    f32 = jnp.float32
    held, rank, columns = mc_ref.shape
    pairs = rank // 2
    spread = row_spread(rank)

    def per_pair(values):
        return jnp.max(jnp.where(spread, values, 0.0), axis=0, keepdims=True)

    def per_row(scales):
        return jnp.sum(jnp.where(spread, scales, 0.0), axis=1, keepdims=True)

    for j in range(held):
        gradient = total_ref[j * rank : (j + 1) * rank, :]
        moment, second, direction = moments(j, aux_ref, gradient, mc_ref, vc_ref, spread)
        keep = trained_row(aux_ref, held, j, moment.shape)
        keep_row = trained_row(aux_ref, held, j, (1, pairs))
        m_new = per_pair(jnp.max(jnp.abs(moment), axis=1, keepdims=True)) + scale_eps
        v_new = per_pair(jnp.max(second, axis=1, keepdims=True)) + scale_eps
        dir_ref[j] = jnp.where(keep, direction, 0.0)
        m_code, v_code = moment / per_row(m_new), second / per_row(v_new)
        mc_out[j] = jnp.where(keep, m_code, mc_ref[j].astype(f32)).astype(mc_out.dtype)
        vc_out[j] = jnp.where(keep, v_code, vc_ref[j].astype(f32)).astype(vc_out.dtype)
        ms_out[j : j + 1, :] = jnp.where(keep_row, m_new, aux_ref[j : j + 1, :pairs])
        vs_out[j : j + 1, :] = jnp.where(keep_row, v_new, aux_ref[held + j : held + j + 1, :pairs])


def state(aux, total, m_code, v_code):
    f32 = jnp.float32
    like = jax.ShapeDtypeStruct
    scales = like((m_code.shape[0], m_code.shape[1] // 2), f32)
    return pl.pallas_call(
        state_kernel,
        out_shape=(
            like(m_code.shape, f32),
            like(m_code.shape, m_code.dtype),
            scales,
            like(v_code.shape, v_code.dtype),
            scales,
        ),
        in_specs=[VMEM] * 4,
        out_specs=(VMEM,) * 5,
        compiler_params=GRANT,
        name="state",
    )(aux, total, m_code, v_code)


def on_device(
    features, cotangent, adapter_ids, slot_of, active_ids, step_counts,
    weight, m_code, m_scale, v_code, v_scale,
):
    columns = features.shape[1]
    held, rank = weight.shape[0], weight.shape[1]
    half = held * rank
    chips = lax.axis_size(("x", "z"))
    replicas = lax.axis_size("replica")
    core = lax.axis_index("core").astype(jnp.int32).reshape(1)
    owner = lax.axis_index(("x", "z", "core")).astype(jnp.int32).reshape(1)
    small = (
        adapter_ids.reshape(1, -1), slot_of.reshape(1, -1), active_ids.reshape(1, -1), step_counts.reshape(1, -1),
        m_scale.reshape(held, -1), v_scale.reshape(held, -1),
    )

    def exchange(slots, offset):
        sent, aux = pack(slots, chips, core, owner, offset, small, cotangent.T, features)
        received = lax.all_to_all(sent, ("x", "z"), split_axis=0, concat_axis=0, tiled=True)
        return partial_gradients(slots, offset, received, half, columns), aux

    def another(carry):
        own, other, rank_next = carry
        (more_own, more_other, rank_next), _ = exchange(1, rank_next)
        return own + more_own, other + more_other, rank_next

    carry, aux = exchange(FIRST, jnp.zeros((1,), jnp.int32))
    own, other, _ = lax.while_loop(lambda carry: carry[2][0] > 0, another, carry)
    other = lax.ppermute(other, "core", [(0, 1), (1, 0)])
    copies, total = serve(replicas, aux, own, other, weight, m_code, v_code)
    parts = lax.all_to_all(copies, "replica", split_axis=0, concat_axis=0, tiled=True)
    direction, m_new, ms_new, v_new, vs_new = state(aux, total, m_code, v_code)
    served = assemble(parts)
    return (
        direction, m_new, ms_new.reshape(m_scale.shape), v_new, vs_new.reshape(v_scale.shape), served,
    )


def solution(mesh):
    owners, replicas = mesh.devices.shape
    fine = Mesh(mesh.devices.reshape(4, owners // 8, 2, replicas), ("x", "z", "core", "replica"))
    owner = ("x", "z", "core")
    block = P(owner, None, "replica")
    return jax.shard_map(
        on_device,
        mesh=fine,
        in_specs=(
            P(owner, "replica"), P(owner, None), P(owner, None), P(), P(), P(owner),
            block, block, block, block, block,
        ),
        out_specs=(block, block, block, block, block, P(owner, None, None)),
        check_vma=False,
    )
```

```python
import functools

import jax
import jax.numpy as jnp
from jax import lax
from jax.experimental import pallas as pl
from jax.experimental.pallas import tpu as pltpu
from jax.sharding import Mesh
from jax.sharding import PartitionSpec as P

beta_one = 0.9
beta_two = 0.999
adam_eps = 1e-08
scale_eps = 1e-06
learn_rate = 0.001
decay_rate = 0.01

LANES = 128
PIECES = 2
FIRST = 6
VMEM = pl.BlockSpec(memory_space=pltpu.VMEM)
SMEM = pl.BlockSpec(memory_space=pltpu.SMEM)
ANY = pl.BlockSpec(memory_space=pl.ANY)
GRANT = pltpu.CompilerParams(vmem_limit_bytes=16 << 20)


def message_rows(slots, blocks):
    rows = slots * blocks + (slots + 1) // 2 + 1
    return -(-rows // 4) * 4


def iota(shape, dim):
    return lax.broadcasted_iota(jnp.int32, shape, dim)


def near_kernel(*refs):
    del refs


def near(*arrays):
    return pl.pallas_call(
        near_kernel,
        out_shape=tuple(jax.ShapeDtypeStruct(a.shape, a.dtype) for a in arrays),
        in_specs=[ANY] * len(arrays),
        out_specs=(ANY,) * len(arrays),
        input_output_aliases={n: n for n in range(len(arrays))},
        compiler_params=GRANT,
        name="near",
    )(*arrays)


def pack_kernel(
    slots, core_ref, owner_ref, offset_ref, ids_ref, slot_ref, act_ref, count_ref, ms_ref, vs_ref, cot_ref, feat_ref,
    out_ref, aux_ref, scr,
):
    rank, tokens = cot_ref.shape
    state_rows = slot_ref.shape[1]
    columns = feat_ref.shape[1]
    chips, tiles = out_ref.shape[0], out_ref.shape[1]
    rows, blocks = tiles * 4, columns // LANES
    held, pairs = ms_ref.shape
    f32, bf16 = jnp.float32, jnp.bfloat16
    dot = functools.partial(jnp.dot, preferred_element_type=f32)
    here, owner, offset = core_ref[0], owner_ref[0], offset_ref[0].astype(f32)

    square = (state_rows, state_rows)
    named = slot_ref[...] == iota(square, 0)
    adapter = jnp.sum(jnp.where(named, iota(square, 1), 0).astype(f32), axis=1, keepdims=True)
    adapter = adapter.astype(jnp.int32)
    trained = jnp.max((act_ref[...] == adapter).astype(f32), axis=1, keepdims=True)
    place = jnp.where(ids_ref[...] == adapter, trained, 0.0).astype(bf16)
    of_chip = (iota((chips, state_rows), 1) // 4 == iota((chips, state_rows), 0)).astype(f32).astype(bf16)
    member = dot(of_chip, place)
    earlier = (iota((tokens, tokens), 0) < iota((tokens, tokens), 1)).astype(f32).astype(bf16)
    before = dot(member.astype(bf16), earlier) - offset
    late = jnp.where((member > 0) & (before >= slots), 1.0, 0.0)
    more = jnp.max(jnp.max(late, axis=1, keepdims=True), axis=0, keepdims=True)
    chosen = jnp.concatenate([jnp.where(before == i, member, 0.0).astype(bf16) for i in range(slots)], axis=0)

    local = (iota((state_rows, LANES), 0) + 2 * here) % 4
    tag = (iota((state_rows, LANES), 1) == rank + local).astype(f32).astype(bf16)
    embed = (iota((rank, LANES), 0) == iota((rank, LANES), 1)).astype(f32).astype(bf16)
    beside = lax.dot_general(
        jnp.concatenate([cot_ref[...], place], axis=0),
        jnp.concatenate([embed, tag], axis=0),
        (((0,), (0,)), ((), ())),
        preferred_element_type=f32,
    )
    beside = dot(chosen, beside.astype(bf16))
    of_slot = [slice(i * chips, (i + 1) * chips) for i in range(slots)]
    lane = iota((chips, LANES), 1)
    tags = jnp.where(lane == 4 * slots, more, 0.0)
    for i in range(slots):
        one = jnp.where((lane >= rank) & (lane < rank + 4), beside[of_slot[i]], 0.0)
        tags = tags + pltpu.roll(one, (LANES - rank + 4 * i) % LANES, 1)
    for p in range((slots + 1) // 2):
        pair = jnp.where(lane < rank, beside[of_slot[2 * p]], 0.0)
        if 2 * p + 1 < slots:
            pair = jnp.where(lane < rank, pair, pltpu.roll(beside[of_slot[2 * p + 1]], rank, 1))
        scr[pl.ds(slots * blocks + p, chips, stride=rows), :] = pair
    for r in range(slots * blocks + (slots + 1) // 2, rows):
        scr[pl.ds(r, chips, stride=rows), :] = tags

    aux_ref[...] = jnp.zeros(aux_ref.shape, f32)
    aux_ref[:held, :pairs] = ms_ref[...]
    aux_ref[held : 2 * held, :pairs] = vs_ref[...]
    count = count_ref[...] + 1
    for at, beta in ((2 * held, beta_one), (2 * held + 1, beta_two)):
        power = jnp.ones(count.shape, f32)
        for bit in range(8):
            power = jnp.where((count >> bit) % 2 == 1, power * beta ** (1 << bit), power)
        aux_ref[at : at + 1, :held] = 1.0 / (1.0 - power)
    state_row = iota((state_rows, held), 0) - held * owner
    mine = jnp.where(state_row == iota((state_rows, held), 1), trained, 0.0)
    aux_ref[2 * held + 2 : 2 * held + 3, :held] = jnp.max(mine, axis=0, keepdims=True)

    moved = dot(chosen, feat_ref[...])
    for i in range(slots):
        for b in range(blocks):
            scr[pl.ds(i * blocks + b, chips, stride=rows), :] = moved[of_slot[i], b * LANES : (b + 1) * LANES]
    out_ref[...] = scr[...].astype(out_ref.dtype).reshape(chips, tiles, 4, LANES)


def pack(slots, chips, core, owner, offset, small, cotangent, features):
    rows = message_rows(slots, features.shape[1] // LANES)
    like = jax.ShapeDtypeStruct
    return pl.pallas_call(
        functools.partial(pack_kernel, slots),
        out_shape=(like((chips, rows // 4, 4, LANES), features.dtype), like((8, LANES), jnp.float32)),
        in_specs=[SMEM] * 3 + [VMEM] * 8,
        out_specs=(VMEM, VMEM),
        scratch_shapes=[pltpu.VMEM((chips * rows, LANES), jnp.float32)],
        compiler_params=GRANT,
        name=f"pack{slots}",
    )(core, owner, offset, *small, cotangent, features)


def grad_kernel(slots, offset_ref, in_ref, own_ref, other_ref, next_ref, scr):
    chips, tiles = in_ref.shape[0], in_ref.shape[1]
    rows = tiles * 4
    half, columns = own_ref.shape
    rank = half // 2
    blocks = columns // LANES
    f32, bf16 = jnp.float32, jnp.bfloat16
    scr[...] = in_ref[...].reshape(chips * rows, LANES).astype(f32)
    low = iota((chips, LANES), 1) < rank
    tags = scr[pl.ds(rows - 1, chips, stride=rows), :]
    more = jnp.max(tags[:, 4 * slots : 4 * slots + 1]) > 0
    next_ref[0] = jnp.where(more, offset_ref[0] + slots, 0)
    weights, wide = [], []
    for i in range(slots):
        pair = scr[pl.ds(slots * blocks + i // 2, chips, stride=rows), :]
        one = jnp.where(low if i % 2 == 0 else ~low, pair, 0.0)
        both = one + pltpu.roll(one, rank, 1)
        h = [tags[:, 4 * i + l : 4 * i + l + 1] for l in range(4)]
        weights.append(
            jnp.concatenate(
                [both * jnp.where(low, h[0], h[1]), both * jnp.where(low, h[2], h[3])], axis=1
            ).astype(bf16)
        )
        wide.append(
            jnp.concatenate(
                [scr[pl.ds(i * blocks + b, chips, stride=rows), :] for b in range(blocks)], axis=1
            ).astype(bf16)
        )
    total = lax.dot_general(
        jnp.concatenate(weights, axis=0),
        jnp.concatenate(wide, axis=0),
        (((0,), (0,)), ((), ())),
        preferred_element_type=f32,
    )
    own_ref[...] = total[:half]
    other_ref[...] = total[half:]


def partial_gradients(slots, offset, received, half, columns):
    chips, tiles = received.shape[0], received.shape[1]
    f32 = jnp.float32
    return pl.pallas_call(
        functools.partial(grad_kernel, slots),
        out_shape=(
            jax.ShapeDtypeStruct((half, columns), f32),
            jax.ShapeDtypeStruct((half, columns), f32),
            jax.ShapeDtypeStruct((1,), jnp.int32),
        ),
        in_specs=[SMEM, VMEM],
        out_specs=(VMEM, VMEM, SMEM),
        scratch_shapes=[pltpu.VMEM((chips * tiles * 4, LANES), f32)],
        compiler_params=GRANT,
        name=f"grad{slots}",
    )(offset, received)


def moments(j, aux_ref, gradient, mc_ref, vc_ref, spread, at=slice(None)):
    f32 = jnp.float32
    held, rank, _ = mc_ref.shape
    pairs = rank // 2

    def per_row(at):
        return jnp.sum(jnp.where(spread, aux_ref[at : at + 1, :pairs], 0.0), axis=1, keepdims=True)

    moment = mc_ref[j, :, at].astype(f32) * (beta_one * per_row(j)) + (1.0 - beta_one) * gradient
    second = vc_ref[j, :, at].astype(f32) * (beta_two * per_row(held + j)) + (1.0 - beta_two) * gradient * gradient
    inverse_one = aux_ref[2 * held : 2 * held + 1, j : j + 1]
    inverse_two = aux_ref[2 * held + 1 : 2 * held + 2, j : j + 1]
    direction = (moment * inverse_one) / (jnp.sqrt(second * inverse_two) + adam_eps)
    return moment, second, direction


def row_spread(rank):
    return iota((rank, rank // 2), 0) // 2 == iota((rank, rank // 2), 1)


def trained_row(aux_ref, held, j, shape):
    return jnp.broadcast_to(aux_ref[2 * held + 2 : 2 * held + 3, j : j + 1], shape) > 0


def serve_kernel(aux_ref, own_ref, other_ref, weight_ref, mc_ref, vc_ref, served_hbm, total_ref, out_ref, sems):
    held, rank, columns = weight_ref.shape
    spread = row_spread(rank)
    width = columns // PIECES
    sends = []
    for n in range(held * PIECES):
        j, first = n // PIECES, n % PIECES * width
        rows, at = slice(j * rank, (j + 1) * rank), slice(first, first + width)
        gradient = own_ref[rows, at] + other_ref[rows, at]
        total_ref[rows, at] = gradient
        _, _, direction = moments(j, aux_ref, gradient, mc_ref, vc_ref, spread, at)
        weight = weight_ref[j, :, at].astype(jnp.float32)
        served = weight - learn_rate * (direction + decay_rate * weight)
        served = jnp.where(trained_row(aux_ref, held, j, weight.shape), served, weight)
        out_ref[j, :, at] = served.astype(out_ref.dtype)
        piece = (slice(None), pl.ds(first, width))
        for r in range(served_hbm.shape[0]):
            send = pltpu.make_async_copy(out_ref.at[j, *piece], served_hbm.at[r, j, *piece], sems.at[n, r])
            send.start()
            sends.append(send)
    for send in sends:
        send.wait()


def serve(replicas, aux, own, other, weight, m_code, v_code):
    held = weight.shape[0]
    like = jax.ShapeDtypeStruct
    return pl.pallas_call(
        serve_kernel,
        out_shape=(like((replicas, *weight.shape), weight.dtype), like(own.shape, jnp.float32)),
        in_specs=[VMEM] * 6,
        out_specs=(ANY, VMEM),
        scratch_shapes=[
            pltpu.VMEM(weight.shape, weight.dtype),
            pltpu.SemaphoreType.DMA((held * PIECES, replicas)),
        ],
        compiler_params=GRANT,
        name="serve",
    )(aux, own, other, weight, m_code, v_code)


def assemble_kernel(parts_ref, out_ref, sems):
    replicas, columns = parts_ref.shape[0], parts_ref.shape[3]
    moves = [
        pltpu.make_async_copy(parts_ref.at[r], out_ref.at[:, :, pl.ds(r * columns, columns)], sems.at[r])
        for r in range(replicas)
    ]
    for move in moves:
        move.start()
    for move in moves:
        move.wait()


def assemble(parts):
    replicas, held, rank, columns = parts.shape
    return pl.pallas_call(
        assemble_kernel,
        out_shape=jax.ShapeDtypeStruct((held, rank, replicas * columns), parts.dtype),
        in_specs=[ANY],
        out_specs=ANY,
        scratch_shapes=[pltpu.SemaphoreType.DMA((replicas,))],
        compiler_params=GRANT,
        name="assemble",
    )(parts)


def state_kernel(
    aux_ref, total_ref, mc_ref, vc_ref, dir_ref, mc_out, ms_out, vc_out, vs_out
):
    f32 = jnp.float32
    held, rank, columns = mc_ref.shape
    pairs = rank // 2
    spread = row_spread(rank)

    def per_pair(values):
        return jnp.max(jnp.where(spread, values, 0.0), axis=0, keepdims=True)

    def per_row(scales):
        return jnp.sum(jnp.where(spread, scales, 0.0), axis=1, keepdims=True)

    for j in range(held):
        gradient = total_ref[j * rank : (j + 1) * rank, :]
        moment, second, direction = moments(j, aux_ref, gradient, mc_ref, vc_ref, spread)
        keep = trained_row(aux_ref, held, j, moment.shape)
        keep_row = trained_row(aux_ref, held, j, (1, pairs))
        m_new = per_pair(jnp.max(jnp.abs(moment), axis=1, keepdims=True)) + scale_eps
        v_new = per_pair(jnp.max(second, axis=1, keepdims=True)) + scale_eps
        dir_ref[j] = jnp.where(keep, direction, 0.0)
        m_code, v_code = moment / per_row(m_new), second / per_row(v_new)
        mc_out[j] = jnp.where(keep, m_code, mc_ref[j].astype(f32)).astype(mc_out.dtype)
        vc_out[j] = jnp.where(keep, v_code, vc_ref[j].astype(f32)).astype(vc_out.dtype)
        ms_out[j : j + 1, :] = jnp.where(keep_row, m_new, aux_ref[j : j + 1, :pairs])
        vs_out[j : j + 1, :] = jnp.where(keep_row, v_new, aux_ref[held + j : held + j + 1, :pairs])


def state(aux, total, m_code, v_code):
    f32 = jnp.float32
    like = jax.ShapeDtypeStruct
    scales = like((m_code.shape[0], m_code.shape[1] // 2), f32)
    return pl.pallas_call(
        state_kernel,
        out_shape=(
            like(m_code.shape, f32),
            like(m_code.shape, m_code.dtype),
            scales,
            like(v_code.shape, v_code.dtype),
            scales,
        ),
        in_specs=[VMEM] * 4,
        out_specs=(VMEM,) * 5,
        compiler_params=GRANT,
        name="state",
    )(aux, total, m_code, v_code)


def on_device(
    features, cotangent, adapter_ids, slot_of, active_ids, step_counts,
    weight, m_code, m_scale, v_code, v_scale,
):
    columns = features.shape[1]
    held, rank = weight.shape[0], weight.shape[1]
    half = held * rank
    chips = lax.axis_size(("x", "z"))
    replicas = lax.axis_size("replica")
    core = lax.axis_index("core").astype(jnp.int32).reshape(1)
    owner = lax.axis_index(("x", "z", "core")).astype(jnp.int32).reshape(1)
    small = (
        adapter_ids.reshape(1, -1), slot_of.reshape(1, -1), active_ids.reshape(1, -1), step_counts.reshape(1, -1),
        m_scale.reshape(held, -1), v_scale.reshape(held, -1),
    )

    *small, cot, close = near(*small, cotangent.T, features)

    def exchange(slots, offset):
        sent, aux = pack(slots, chips, core, owner, offset, small, cot, close)
        received = lax.all_to_all(sent, ("x", "z"), split_axis=0, concat_axis=0, tiled=True)
        return partial_gradients(slots, offset, received, half, columns), aux

    def another(carry):
        own, other, rank_next = carry
        (more_own, more_other, rank_next), _ = exchange(1, rank_next)
        return own + more_own, other + more_other, rank_next

    carry, aux = exchange(FIRST, jnp.zeros((1,), jnp.int32))
    own, other, _ = lax.while_loop(lambda carry: carry[2][0] > 0, another, carry)
    other = lax.ppermute(other, "core", [(0, 1), (1, 0)])
    copies, total = serve(replicas, aux, own, other, weight, m_code, v_code)
    parts = lax.all_to_all(copies, "replica", split_axis=0, concat_axis=0, tiled=True)
    direction, m_new, ms_new, v_new, vs_new = state(aux, total, m_code, v_code)
    served = assemble(parts)
    return (
        direction, m_new, ms_new.reshape(m_scale.shape), v_new, vs_new.reshape(v_scale.shape), served,
    )


def solution(mesh):
    owners, replicas = mesh.devices.shape
    fine = Mesh(mesh.devices.reshape(4, owners // 8, 2, replicas), ("x", "z", "core", "replica"))
    owner = ("x", "z", "core")
    block = P(owner, None, "replica")
    return jax.shard_map(
        on_device,
        mesh=fine,
        in_specs=(
            P(owner, "replica"), P(owner, None), P(owner, None), P(), P(), P(owner),
            block, block, block, block, block,
        ),
        out_specs=(block, block, block, block, block, P(owner, None, None)),
        check_vma=False,
    )
```

```python
import functools

import jax
import jax.numpy as jnp
from jax import lax
from jax.experimental import pallas as pl
from jax.experimental.pallas import tpu as pltpu
from jax.sharding import Mesh
from jax.sharding import PartitionSpec as P

beta_one = 0.9
beta_two = 0.999
adam_eps = 1e-08
scale_eps = 1e-06
learn_rate = 0.001
decay_rate = 0.01

LANES = 128
PIECES = 4
FIRST = 6
VMEM = pl.BlockSpec(memory_space=pltpu.VMEM)
SMEM = pl.BlockSpec(memory_space=pltpu.SMEM)
ANY = pl.BlockSpec(memory_space=pl.ANY)
GRANT = pltpu.CompilerParams(vmem_limit_bytes=16 << 20)


def message_rows(slots, blocks):
    rows = slots * blocks + (slots + 1) // 2 + 1
    return -(-rows // 4) * 4


def iota(shape, dim):
    return lax.broadcasted_iota(jnp.int32, shape, dim)


def near_kernel(*refs):
    del refs


def near(*arrays):
    return pl.pallas_call(
        near_kernel,
        out_shape=tuple(jax.ShapeDtypeStruct(a.shape, a.dtype) for a in arrays),
        in_specs=[ANY] * len(arrays),
        out_specs=(ANY,) * len(arrays),
        input_output_aliases={n: n for n in range(len(arrays))},
        compiler_params=GRANT,
        name="near",
    )(*arrays)


def pack_kernel(
    slots, core_ref, owner_ref, offset_ref, ids_ref, slot_ref, act_ref, count_ref, ms_ref, vs_ref, cot_ref, feat_ref,
    out_ref, aux_ref, scr,
):
    rank, tokens = cot_ref.shape
    state_rows = slot_ref.shape[1]
    columns = feat_ref.shape[1]
    chips, tiles = out_ref.shape[0], out_ref.shape[1]
    rows, blocks = tiles * 4, columns // LANES
    held, pairs = ms_ref.shape
    f32, bf16 = jnp.float32, jnp.bfloat16
    dot = functools.partial(jnp.dot, preferred_element_type=f32)
    here, owner, offset = core_ref[0], owner_ref[0], offset_ref[0].astype(f32)

    square = (state_rows, state_rows)
    named = slot_ref[...] == iota(square, 0)
    adapter = jnp.sum(jnp.where(named, iota(square, 1), 0).astype(f32), axis=1, keepdims=True)
    adapter = adapter.astype(jnp.int32)
    trained = jnp.max((act_ref[...] == adapter).astype(f32), axis=1, keepdims=True)
    place = jnp.where(ids_ref[...] == adapter, trained, 0.0).astype(bf16)
    of_chip = (iota((chips, state_rows), 1) // 4 == iota((chips, state_rows), 0)).astype(f32).astype(bf16)
    member = dot(of_chip, place)
    earlier = (iota((tokens, tokens), 0) < iota((tokens, tokens), 1)).astype(f32).astype(bf16)
    before = dot(member.astype(bf16), earlier) - offset
    late = jnp.where((member > 0) & (before >= slots), 1.0, 0.0)
    more = jnp.max(jnp.max(late, axis=1, keepdims=True), axis=0, keepdims=True)
    chosen = jnp.concatenate([jnp.where(before == i, member, 0.0).astype(bf16) for i in range(slots)], axis=0)

    local = (iota((state_rows, LANES), 0) + 2 * here) % 4
    tag = (iota((state_rows, LANES), 1) == rank + local).astype(f32).astype(bf16)
    embed = (iota((rank, LANES), 0) == iota((rank, LANES), 1)).astype(f32).astype(bf16)
    beside = lax.dot_general(
        jnp.concatenate([cot_ref[...], place], axis=0),
        jnp.concatenate([embed, tag], axis=0),
        (((0,), (0,)), ((), ())),
        preferred_element_type=f32,
    )
    beside = dot(chosen, beside.astype(bf16))
    of_slot = [slice(i * chips, (i + 1) * chips) for i in range(slots)]
    lane = iota((chips, LANES), 1)
    tags = jnp.where(lane == 4 * slots, more, 0.0)
    for i in range(slots):
        one = jnp.where((lane >= rank) & (lane < rank + 4), beside[of_slot[i]], 0.0)
        tags = tags + pltpu.roll(one, (LANES - rank + 4 * i) % LANES, 1)
    for p in range((slots + 1) // 2):
        pair = jnp.where(lane < rank, beside[of_slot[2 * p]], 0.0)
        if 2 * p + 1 < slots:
            pair = jnp.where(lane < rank, pair, pltpu.roll(beside[of_slot[2 * p + 1]], rank, 1))
        scr[pl.ds(slots * blocks + p, chips, stride=rows), :] = pair
    for r in range(slots * blocks + (slots + 1) // 2, rows):
        scr[pl.ds(r, chips, stride=rows), :] = tags

    aux_ref[...] = jnp.zeros(aux_ref.shape, f32)
    aux_ref[:held, :pairs] = ms_ref[...]
    aux_ref[held : 2 * held, :pairs] = vs_ref[...]
    count = count_ref[...] + 1
    for at, beta in ((2 * held, beta_one), (2 * held + 1, beta_two)):
        power = jnp.ones(count.shape, f32)
        for bit in range(8):
            power = jnp.where((count >> bit) % 2 == 1, power * beta ** (1 << bit), power)
        aux_ref[at : at + 1, :held] = 1.0 / (1.0 - power)
    state_row = iota((state_rows, held), 0) - held * owner
    mine = jnp.where(state_row == iota((state_rows, held), 1), trained, 0.0)
    aux_ref[2 * held + 2 : 2 * held + 3, :held] = jnp.max(mine, axis=0, keepdims=True)

    moved = dot(chosen, feat_ref[...])
    for i in range(slots):
        for b in range(blocks):
            scr[pl.ds(i * blocks + b, chips, stride=rows), :] = moved[of_slot[i], b * LANES : (b + 1) * LANES]
    out_ref[...] = scr[...].astype(out_ref.dtype).reshape(chips, tiles, 4, LANES)


def pack(slots, chips, core, owner, offset, small, cotangent, features):
    rows = message_rows(slots, features.shape[1] // LANES)
    like = jax.ShapeDtypeStruct
    return pl.pallas_call(
        functools.partial(pack_kernel, slots),
        out_shape=(like((chips, rows // 4, 4, LANES), features.dtype), like((8, LANES), jnp.float32)),
        in_specs=[SMEM] * 3 + [VMEM] * 8,
        out_specs=(VMEM, VMEM),
        scratch_shapes=[pltpu.VMEM((chips * rows, LANES), jnp.float32)],
        compiler_params=GRANT,
        name=f"pack{slots}",
    )(core, owner, offset, *small, cotangent, features)


def grad_kernel(slots, offset_ref, in_ref, own_ref, other_ref, next_ref, scr):
    chips, tiles = in_ref.shape[0], in_ref.shape[1]
    rows = tiles * 4
    half, columns = own_ref.shape
    rank = half // 2
    blocks = columns // LANES
    f32, bf16 = jnp.float32, jnp.bfloat16
    scr[...] = in_ref[...].reshape(chips * rows, LANES).astype(f32)
    low = iota((chips, LANES), 1) < rank
    tags = scr[pl.ds(rows - 1, chips, stride=rows), :]
    more = jnp.max(tags[:, 4 * slots : 4 * slots + 1]) > 0
    next_ref[0] = jnp.where(more, offset_ref[0] + slots, 0)
    weights, wide = [], []
    for i in range(slots):
        pair = scr[pl.ds(slots * blocks + i // 2, chips, stride=rows), :]
        one = jnp.where(low if i % 2 == 0 else ~low, pair, 0.0)
        both = one + pltpu.roll(one, rank, 1)
        h = [tags[:, 4 * i + l : 4 * i + l + 1] for l in range(4)]
        weights.append(
            jnp.concatenate(
                [both * jnp.where(low, h[0], h[1]), both * jnp.where(low, h[2], h[3])], axis=1
            ).astype(bf16)
        )
        wide.append(
            jnp.concatenate(
                [scr[pl.ds(i * blocks + b, chips, stride=rows), :] for b in range(blocks)], axis=1
            ).astype(bf16)
        )
    total = lax.dot_general(
        jnp.concatenate(weights, axis=0),
        jnp.concatenate(wide, axis=0),
        (((0,), (0,)), ((), ())),
        preferred_element_type=f32,
    )
    own_ref[...] = total[:half]
    other_ref[...] = total[half:]


def partial_gradients(slots, offset, received, half, columns):
    chips, tiles = received.shape[0], received.shape[1]
    f32 = jnp.float32
    return pl.pallas_call(
        functools.partial(grad_kernel, slots),
        out_shape=(
            jax.ShapeDtypeStruct((half, columns), f32),
            jax.ShapeDtypeStruct((half, columns), f32),
            jax.ShapeDtypeStruct((1,), jnp.int32),
        ),
        in_specs=[SMEM, VMEM],
        out_specs=(VMEM, VMEM, SMEM),
        scratch_shapes=[pltpu.VMEM((chips * tiles * 4, LANES), f32)],
        compiler_params=GRANT,
        name=f"grad{slots}",
    )(offset, received)


def moments(j, aux_ref, gradient, mc_ref, vc_ref, spread, at=slice(None)):
    f32 = jnp.float32
    held, rank, _ = mc_ref.shape
    pairs = rank // 2

    def per_row(at):
        return jnp.sum(jnp.where(spread, aux_ref[at : at + 1, :pairs], 0.0), axis=1, keepdims=True)

    moment = mc_ref[j, :, at].astype(f32) * (beta_one * per_row(j)) + (1.0 - beta_one) * gradient
    second = vc_ref[j, :, at].astype(f32) * (beta_two * per_row(held + j)) + (1.0 - beta_two) * gradient * gradient
    inverse_one = aux_ref[2 * held : 2 * held + 1, j : j + 1]
    inverse_two = aux_ref[2 * held + 1 : 2 * held + 2, j : j + 1]
    direction = (moment * inverse_one) / (jnp.sqrt(second * inverse_two) + adam_eps)
    return moment, second, direction


def row_spread(rank):
    return iota((rank, rank // 2), 0) // 2 == iota((rank, rank // 2), 1)


def trained_row(aux_ref, held, j, shape):
    return jnp.broadcast_to(aux_ref[2 * held + 2 : 2 * held + 3, j : j + 1], shape) > 0


def serve_kernel(aux_ref, own_ref, other_ref, weight_ref, mc_ref, vc_ref, served_hbm, total_ref, out_ref, sems):
    held, rank, columns = weight_ref.shape
    spread = row_spread(rank)
    width = columns // PIECES
    sends = []
    for n in range(held * PIECES):
        j, first = n // PIECES, n % PIECES * width
        rows, at = slice(j * rank, (j + 1) * rank), slice(first, first + width)
        gradient = own_ref[rows, at] + other_ref[rows, at]
        total_ref[rows, at] = gradient
        _, _, direction = moments(j, aux_ref, gradient, mc_ref, vc_ref, spread, at)
        weight = weight_ref[j, :, at].astype(jnp.float32)
        served = weight - learn_rate * (direction + decay_rate * weight)
        served = jnp.where(trained_row(aux_ref, held, j, weight.shape), served, weight)
        out_ref[j, :, at] = served.astype(out_ref.dtype)
        piece = (slice(None), pl.ds(first, width))
        for r in range(served_hbm.shape[0]):
            send = pltpu.make_async_copy(out_ref.at[j, *piece], served_hbm.at[r, j, *piece], sems.at[n, r])
            send.start()
            sends.append(send)
    for send in sends:
        send.wait()


def serve(replicas, aux, own, other, weight, m_code, v_code):
    held = weight.shape[0]
    like = jax.ShapeDtypeStruct
    return pl.pallas_call(
        serve_kernel,
        out_shape=(like((replicas, *weight.shape), weight.dtype), like(own.shape, jnp.float32)),
        in_specs=[VMEM] * 6,
        out_specs=(ANY, VMEM),
        scratch_shapes=[
            pltpu.VMEM(weight.shape, weight.dtype),
            pltpu.SemaphoreType.DMA((held * PIECES, replicas)),
        ],
        compiler_params=GRANT,
        name="serve",
    )(aux, own, other, weight, m_code, v_code)


def assemble_kernel(parts_ref, out_ref, sems):
    replicas, columns = parts_ref.shape[0], parts_ref.shape[3]
    moves = [
        pltpu.make_async_copy(parts_ref.at[r], out_ref.at[:, :, pl.ds(r * columns, columns)], sems.at[r])
        for r in range(replicas)
    ]
    for move in moves:
        move.start()
    for move in moves:
        move.wait()


def assemble(parts):
    replicas, held, rank, columns = parts.shape
    return pl.pallas_call(
        assemble_kernel,
        out_shape=jax.ShapeDtypeStruct((held, rank, replicas * columns), parts.dtype),
        in_specs=[ANY],
        out_specs=ANY,
        scratch_shapes=[pltpu.SemaphoreType.DMA((replicas,))],
        compiler_params=GRANT,
        name="assemble",
    )(parts)


def state_kernel(
    aux_ref, total_ref, mc_ref, vc_ref, dir_ref, mc_out, ms_out, vc_out, vs_out
):
    f32 = jnp.float32
    held, rank, columns = mc_ref.shape
    pairs = rank // 2
    spread = row_spread(rank)

    def per_pair(values):
        return jnp.max(jnp.where(spread, values, 0.0), axis=0, keepdims=True)

    def per_row(scales):
        return jnp.sum(jnp.where(spread, scales, 0.0), axis=1, keepdims=True)

    for j in range(held):
        gradient = total_ref[j * rank : (j + 1) * rank, :]
        moment, second, direction = moments(j, aux_ref, gradient, mc_ref, vc_ref, spread)
        keep = trained_row(aux_ref, held, j, moment.shape)
        keep_row = trained_row(aux_ref, held, j, (1, pairs))
        m_new = per_pair(jnp.max(jnp.abs(moment), axis=1, keepdims=True)) + scale_eps
        v_new = per_pair(jnp.max(second, axis=1, keepdims=True)) + scale_eps
        dir_ref[j] = jnp.where(keep, direction, 0.0)
        m_code, v_code = moment / per_row(m_new), second / per_row(v_new)
        mc_out[j] = jnp.where(keep, m_code, mc_ref[j].astype(f32)).astype(mc_out.dtype)
        vc_out[j] = jnp.where(keep, v_code, vc_ref[j].astype(f32)).astype(vc_out.dtype)
        ms_out[j : j + 1, :] = jnp.where(keep_row, m_new, aux_ref[j : j + 1, :pairs])
        vs_out[j : j + 1, :] = jnp.where(keep_row, v_new, aux_ref[held + j : held + j + 1, :pairs])


def state(aux, total, m_code, v_code):
    f32 = jnp.float32
    like = jax.ShapeDtypeStruct
    scales = like((m_code.shape[0], m_code.shape[1] // 2), f32)
    return pl.pallas_call(
        state_kernel,
        out_shape=(
            like(m_code.shape, f32),
            like(m_code.shape, m_code.dtype),
            scales,
            like(v_code.shape, v_code.dtype),
            scales,
        ),
        in_specs=[VMEM] * 4,
        out_specs=(VMEM,) * 5,
        compiler_params=GRANT,
        name="state",
    )(aux, total, m_code, v_code)


def on_device(
    features, cotangent, adapter_ids, slot_of, active_ids, step_counts,
    weight, m_code, m_scale, v_code, v_scale,
):
    columns = features.shape[1]
    held, rank = weight.shape[0], weight.shape[1]
    half = held * rank
    chips = lax.axis_size(("x", "z"))
    replicas = lax.axis_size("replica")
    core = lax.axis_index("core").astype(jnp.int32).reshape(1)
    owner = lax.axis_index(("x", "z", "core")).astype(jnp.int32).reshape(1)
    small = (
        adapter_ids.reshape(1, -1), slot_of.reshape(1, -1), active_ids.reshape(1, -1), step_counts.reshape(1, -1),
        m_scale.reshape(held, -1), v_scale.reshape(held, -1),
    )

    *small, cot, close = near(*small, cotangent.T, features)

    def exchange(slots, offset):
        sent, aux = pack(slots, chips, core, owner, offset, small, cot, close)
        received = lax.all_to_all(sent, ("x", "z"), split_axis=0, concat_axis=0, tiled=True)
        return partial_gradients(slots, offset, received, half, columns), aux

    def another(carry):
        own, other, rank_next = carry
        (more_own, more_other, rank_next), _ = exchange(1, rank_next)
        return own + more_own, other + more_other, rank_next

    carry, aux = exchange(FIRST, jnp.zeros((1,), jnp.int32))
    own, other, _ = lax.while_loop(lambda carry: carry[2][0] > 0, another, carry)
    other = lax.ppermute(other, "core", [(0, 1), (1, 0)])
    copies, total = serve(replicas, aux, own, other, weight, m_code, v_code)
    parts = lax.all_to_all(copies, "replica", split_axis=0, concat_axis=0, tiled=True)
    direction, m_new, ms_new, v_new, vs_new = state(aux, total, m_code, v_code)
    served = assemble(parts)
    return (
        direction, m_new, ms_new.reshape(m_scale.shape), v_new, vs_new.reshape(v_scale.shape), served,
    )


def solution(mesh):
    owners, replicas = mesh.devices.shape
    fine = Mesh(mesh.devices.reshape(4, owners // 8, 2, replicas), ("x", "z", "core", "replica"))
    owner = ("x", "z", "core")
    block = P(owner, None, "replica")
    return jax.shard_map(
        on_device,
        mesh=fine,
        in_specs=(
            P(owner, "replica"), P(owner, None), P(owner, None), P(), P(), P(owner),
            block, block, block, block, block,
        ),
        out_specs=(block, block, block, block, block, P(owner, None, None)),
        check_vma=False,
    )
```
